128 devices in a mesh: gx: 8 (over x, core), gy: 16 (over z, y).
Axes of the slice: x: 4, y: 4, z: 4, core: 2. Of those that a mesh axis runs over, the one named last changes fastest.
Arguments:
- atm_fields: bfloat16 [786432, 128], P(('gx', 'gy')), may hold values from -6 to 6
- atm_pos: int32 [3072], replicated, may hold values from 0 to 3071, as said below
- tile_src: int32 [20480], P(('gx', 'gy')), may hold values from 0 to 3071, as said below
- tile_tgt: int32 [20480], P(('gx', 'gy')), may hold values from 0 to 1
- tile_count: int32 [128], P(('gx', 'gy')), may hold values from 128 to 160, as said below
- tile_weight: bfloat16 [20480, 256, 256], P(('gx', 'gy')), may hold values from -0.0625 to 0.0625
- ocean_state: bfloat16 [256, 256, 128], P('gy', 'gx'), may hold values from -6 to 6
- land_mask: int32 [256, 256], P('gy', 'gx'), may hold values 0 or 1
- mixing: float32 [128], replicated, may hold values from 0.03 to 0.24
Outputs:
- ocean_next: bfloat16 [256, 256, 128], P('gy', 'gx')
The draws below stay inside these ranges and needn't reach their ends.
Inputs may be any that keep to these rules, and one draw needn't show every extreme that they name: `atm_pos`: a permutation of the block positions. `tile_src`: among the 160 slots of one device, live or not, no owning device (atm_pos of the block // 24) is named by more than 2 slots; on every device with 160 live slots some owner is named by exactly 2. `tile_count`: live slots are a device's first ones; one device has exactly 160.
All inputs are finite; a program needn't handle non-finite values. No bound on the sum of `land_mask` on one device may be relied on, other than what follows from the above.
Results may differ from the reference program's by a relative error of at most 0.001.
Values may be sent and summed in bfloat16 or wider, within the bound.
A program may use at most 128 MiB of HBM per device.

```python
import math
import jax
import jax.numpy as jnp
from jax import lax

TILE_ROWS = 256
CHANNELS = 128
ATM_BLOCKS = 24
TILE_SLOTS = 160
LAT_CELLS = 16
LON_CELLS = 32
RECV_SLOTS = 256
TARGET_BLOCKS = 2
ALL_BLOCKS = 3072
ALL_TILES = 20480
LATITUDES = 256
LONGITUDES = 256
N_GX = 8
N_GY = 16
DEVICES = 128


def block_order(key):
    return jax.random.permutation(jax.random.fold_in(key, 11), ATM_BLOCKS * DEVICES).astype(jnp.int32)


def draw_atm_pos(key, part):
    return block_order(key)


def draw_tile_src(key, part):
    ordering = block_order(key)
    inverse = jnp.argsort(ordering, stable=True).astype(jnp.int32)
    per_peer = RECV_SLOTS // DEVICES
    device_keys = jax.random.split(jax.random.fold_in(key, 23), DEVICES)

    def one_device(device_key):
        first_key, second_key, third_key = jax.random.split(device_key, 3)
        owner_table = jax.random.permutation(first_key, DEVICES).astype(jnp.int32)
        owners = owner_table[jnp.arange(TILE_SLOTS, dtype=jnp.int32) // per_peer]
        owners = jax.random.permutation(second_key, owners)
        local_slot = jax.random.randint(third_key, (TILE_SLOTS,), 0, ATM_BLOCKS, dtype=jnp.int32)
        return inverse[owners * ATM_BLOCKS + local_slot]
    return jax.vmap(one_device)(device_keys).reshape(DEVICES * TILE_SLOTS).astype(jnp.int32)


def draw_tile_count(key, part):
    first_key, second_key = jax.random.split(jax.random.fold_in(key, 37))
    lowest = TILE_SLOTS - TILE_SLOTS // 5
    counts = jax.random.randint(first_key, (DEVICES,), lowest, TILE_SLOTS + 1, dtype=jnp.int32)
    busiest = jax.random.randint(second_key, (), 0, DEVICES, dtype=jnp.int32)
    return jnp.where(jnp.arange(DEVICES, dtype=jnp.int32) == busiest, TILE_SLOTS, counts).astype(jnp.int32)


def with_ends(entries, stream_key, least, largest):
    index_at = [jax.random.randint(jax.random.fold_in(stream_key, axis), (), 0, length) for axis, length in enumerate(entries.shape)]
    main_axis = entries.shape.index(max(entries.shape))
    beside = index_at[:main_axis] + [(index_at[main_axis] + 1) % entries.shape[main_axis]] + index_at[main_axis + 1:]
    return entries.at[tuple(index_at)].set(least).at[tuple(beside)].set(largest)


def level_of(key, shape, cuts, smallest, high):
    level, own = 1.0, jax.random.fold_in(key, 6)
    for axis_at, blocks in cuts:
        draws = jnp.exp(jax.random.uniform(jax.random.fold_in(own, axis_at), (blocks,), jnp.float32, smallest / len(cuts), high / len(cuts)))
        level = level * jnp.repeat(draws, shape[axis_at] // blocks).reshape([-1 if axis == axis_at else 1 for axis in range(len(shape))])
    return level


def bell_draw(stream_key, extent, width, bound, cuts=(), kind=jnp.bfloat16):
    entries = jax.random.normal(stream_key, extent, jnp.float32) * width
    if len(cuts) > 0:
        entries = level_of(stream_key, extent, cuts, -0.22, 0.18) * entries
    return jnp.clip(entries, min=-bound, max=bound).astype(kind)


def setup_inputs(seed: int = 0) -> dict:
    arg_keys = jax.random.split(jax.random.key(seed), 10)
    return {
        "atm_fields": bell_draw(arg_keys[0], (ALL_BLOCKS * TILE_ROWS, CHANNELS), 1.0, 6.0, ((0, 128),)),
        "atm_pos": draw_atm_pos(jax.random.fold_in(arg_keys[9], 71), 0),
        "tile_src": draw_tile_src(jax.random.fold_in(arg_keys[9], 71), 0),
        "tile_tgt": with_ends(jax.random.randint(arg_keys[3], (ALL_TILES,), 0, TARGET_BLOCKS), jax.random.fold_in(arg_keys[3], 1), 0, TARGET_BLOCKS - 1).astype(jnp.int32),
        "tile_count": draw_tile_count(jax.random.fold_in(arg_keys[9], 71), 0),
        "tile_weight": bell_draw(arg_keys[5], (ALL_TILES, TILE_ROWS, TILE_ROWS), (TILE_ROWS * TILE_SLOTS // 4) ** -0.5, 0.0625, ((0, 128),)),
        "ocean_state": bell_draw(arg_keys[6], (LATITUDES, LONGITUDES, CHANNELS), 1.0, 6.0, ((0, 16), (1, 8))),
        "land_mask": with_ends((jax.random.randint(arg_keys[7], (LATITUDES, LONGITUDES), 0, 4) < 3).astype(jnp.int32), jax.random.fold_in(arg_keys[7], 1), 0, 1),
        "mixing": jnp.clip(jnp.exp(jax.random.uniform(arg_keys[8], (CHANNELS,), jnp.float32, math.log(0.03), math.log(0.24))), 0.03, 0.24),
    }


def neighbours(field):
    west_side = jnp.roll(field, 1, axis=1)
    east_side = jnp.roll(field, -1, axis=1)
    south_side = jnp.concatenate([jnp.zeros_like(field[:1]), field[:-1]], axis=0)
    north_side = jnp.concatenate([field[1:], jnp.flip(field[-1:], axis=1)], axis=0)
    return (west_side, east_side, south_side, north_side)


def reference(atm_fields, atm_pos, tile_src, tile_tgt, tile_count, tile_weight, ocean_state, land_mask, mixing):
    devices = N_GX * N_GY
    block_table = atm_fields.reshape(ATM_BLOCKS * devices, TILE_ROWS, CHANNELS)

    def remap_device(pieces):
        weights, sources, targets, tile_live = pieces
        gathered = block_table[atm_pos[sources]].astype(jnp.float32)
        partial_sum = jnp.einsum("tij,tjc->tic", weights.astype(jnp.float32), gathered, precision=lax.Precision.HIGHEST)
        active = jnp.arange(TILE_SLOTS, dtype=jnp.int32) < tile_live
        select = ((targets[:, None] == jnp.arange(TARGET_BLOCKS, dtype=jnp.int32)[None, :]) & active[:, None]).astype(jnp.float32)
        summed = jnp.einsum("tb,tic->bic", select, partial_sum, precision=lax.Precision.HIGHEST)
        return summed.reshape(LAT_CELLS, LON_CELLS, CHANNELS)

    remapped = lax.map(remap_device, (tile_weight.reshape(devices, TILE_SLOTS, TILE_ROWS, TILE_ROWS), tile_src.reshape(devices, TILE_SLOTS), tile_tgt.reshape(devices, TILE_SLOTS), tile_count))
    forcing = remapped.reshape(N_GX, N_GY, LAT_CELLS, LON_CELLS, CHANNELS).transpose(1, 2, 0, 3, 4)
    forcing = forcing.reshape(N_GY * LAT_CELLS, N_GX * LON_CELLS, CHANNELS)
    center = ocean_state.astype(jnp.float32)
    wet_mask = land_mask.astype(jnp.float32)
    diffusion = jnp.zeros_like(center)
    for side_state, side_mask in zip(neighbours(center), neighbours(wet_mask)):
        diffusion = diffusion + side_mask[..., None] * (side_state - center)
    result = wet_mask[..., None] * (center + forcing + mixing * diffusion)
    return result.astype(jnp.bfloat16)
```

```python
import functools

import jax
import jax.numpy as jnp
from jax import lax
from jax.experimental import pallas as pl
from jax.experimental.pallas import tpu as pltpu
from jax.sharding import PartitionSpec as P

MESH = pl.DeviceIdType.MESH
ROWS = 256
CHANNELS = 128
BLOCKS = 24
RING = 4
CORES = 2
CLASSES = ((0, 96, "xyz"), (96, 80, "yzx"), (176, 80, "zxy"))
FAR = (1, 3, 2)
GROUP = 8
DEPTH = 4


def digit(axis, value):
    return {"x": value // 32, "z": value // 4 % 4, "y": value % 4}[axis]


def peer(axis, offset, flip=0):
    gx, gy = lax.axis_index("gx"), lax.axis_index("gy")
    x, core, z, y = gx // 2, gx % 2, gy // 4, gy % 4
    if axis == "x":
        x = (x + offset) % RING
    if axis == "y":
        y = (y + offset) % RING
    if axis == "z":
        z = (z + offset) % RING
    core = (core + flip) % CORES
    return (x * 2 + core, z * 4 + y)


def slot_of(distance, core, rank):
    return (
        ((distance["x"] * CORES + core) * RING + distance["z"]) * RING + distance["y"]
    ) * 2 + rank


def exchange_kernel(ask, atm, final, *scratch):
    gathered, sent, relayed, first, second = (scratch[3 * i : 3 * i + 3] for i in range(5))
    table, ask_sem, ask_s, ask_r, mid_s, mid_r, smem_sem, own_sem, ag_s, ag_r, p2_s, p2_r, p3_s, p3_r = scratch[15:]

    barrier = pltpu.get_barrier_semaphore()
    neighbours = [(a, o, f) for a in "xyz" for o in (1, 2, 3) for f in (0, 1)] + [("x", 0, 1)]
    for axis, offset, flip in neighbours:
        pl.semaphore_signal(barrier, 1, device_id=peer(axis, offset, flip), device_id_type=MESH)
    pl.semaphore_wait(barrier, len(neighbours))

    def remote(src, dst, send, recv, target):
        copy = pltpu.make_async_remote_copy(
            src_ref=src, dst_ref=dst, send_sem=send, recv_sem=recv, device_id=target, device_id_type=MESH
        )
        copy.start()
        return copy

    asks, mids, owns, rings, p2s, p3s = [], [], [], [], [], []
    for c, (_, _, order) in enumerate(CLASSES):
        local = pltpu.make_async_copy(ask, first[c].at[0], ask_sem.at[c])
        local.start()
        asks.append([local])
        for lane in range(1, RING * CORES):
            o3, flip = lane // CORES, lane % CORES
            asks[c].append(
                remote(ask, first[c].at[lane], ask_s.at[c, lane], ask_r.at[c, lane], peer(order[2], -o3, flip))
            )
    for c, (start, size, order) in enumerate(CLASSES):
        block = atm.at[:, pl.ds(start, size)]
        rings.append(
            [remote(block, gathered[c].at[o], ag_s.at[c, o], ag_r.at[c, o], peer(order[0], o)) for o in FAR]
        )
        own = pltpu.make_async_copy(block, gathered[c].at[0], own_sem.at[c])
        own.start()
        owns.append(own)
    for c, (_, _, order) in enumerate(CLASSES):
        for copy in asks[c]:
            copy.wait()
        mids.append(
            [remote(first[c], second[c].at[o], mid_s.at[c, o], mid_r.at[c, o], peer(order[1], -o)) for o in FAR]
        )
        keep = pltpu.make_async_copy(first[c], table.at[c, 0], smem_sem.at[c, 0])
        keep.start()
        mids[c].append(keep)
    for c in range(3):
        for copy in mids[c]:
            copy.wait()
        keeps = []
        for o in FAR:
            keep = pltpu.make_async_copy(second[c].at[o], table.at[c, o], smem_sem.at[c, o])
            keep.start()
            keeps.append(keep)
        for keep in keeps:
            keep.wait()
    for c in range(3):
        owns[c].wait()
        for copy in rings[c]:
            copy.wait()

    def pack(c, o2):
        order = CLASSES[c][2]

        def body(lane, carry):
            o3, flip = lane // CORES, lane % CORES
            for o1 in range(RING):
                for rank in range(2):
                    at = slot_of({order[0]: o1, order[1]: o2, order[2]: o3}, flip, rank)
                    which = table[c, o2, lane, at // 128, at % 128]
                    sent[c][o2, lane, o1, rank] = gathered[c][o1, which]
            return carry

        lax.fori_loop(0, RING * CORES, body, 0)

    def send2(c, o2):
        order = CLASSES[c][2]
        return remote(
            sent[c].at[o2], relayed[c].at[o2], p2_s.at[c, o2], p2_r.at[c, o2], peer(order[1], o2)
        )

    def send3(c, o2):
        start, size, order = CLASSES[c]
        source = sent[c] if o2 == 0 else relayed[c]
        for lane in range(RING * CORES):
            o3, flip = lane // CORES, lane % CORES
            at = {order[0]: slice(None), order[1]: o2, order[2]: o3}
            dst = final.at[at["x"], flip, at["z"], at["y"], :, pl.ds(start, size)]
            src = source.at[o2, lane]
            if lane == 0:
                copy = pltpu.make_async_copy(src, dst, p3_s.at[c, o2, 0])
                copy.start()
                p3s.append(copy)
            else:
                p3s.append(
                    remote(src, dst, p3_s.at[c, o2, lane], p3_r.at[c, o2, lane], peer(order[2], o3, flip))
                )

    steps = [(c, o2) for o2 in FAR + (0,) for c in range(3)]
    pending = {}
    for i, (c, o2) in enumerate(steps + [None]) if False else enumerate(steps):
        pack(c, o2)
        if i > 0:
            cc, oo = steps[i - 1]
            if oo:
                pending[cc, oo] = send2(cc, oo)
            else:
                send3(cc, oo)
    send3(*steps[-1])
    for o2 in FAR:
        for c in range(3):
            pending[c, o2].wait()
            send3(c, o2)
    for copy in p3s:
        copy.wait()


def exchange(ask, atm):
    dma = pltpu.SemaphoreType.DMA
    tables = RING * CORES
    scratch = [pltpu.VMEM((RING, BLOCKS, size, CHANNELS), jnp.bfloat16) for _, size, _ in CLASSES]
    for _ in range(2):
        scratch += [
            pltpu.VMEM((RING, tables, RING, 2, size, CHANNELS), jnp.bfloat16) for _, size, _ in CLASSES
        ]
    scratch += [pltpu.VMEM((tables, 2, 128), jnp.int32) for _ in CLASSES]
    scratch += [pltpu.VMEM((RING, tables, 2, 128), jnp.int32) for _ in CLASSES]
    scratch += [
        pltpu.SMEM((3, RING, tables, 2, 128), jnp.int32),
        dma((3,)),
        dma((3, tables)),
        dma((3, tables)),
        dma((3, RING)),
        dma((3, RING)),
        dma((3, RING)),
        dma((3,)),
        dma((3, RING)),
        dma((3, RING)),
        dma((3, RING)),
        dma((3, RING)),
        dma((3, RING, tables)),
        dma((3, RING, tables)),
    ]
    return pl.pallas_call(
        exchange_kernel,
        out_shape=jax.ShapeDtypeStruct((RING, CORES, RING, RING, 2, ROWS, CHANNELS), jnp.bfloat16),
        in_specs=[pl.BlockSpec(memory_space=pltpu.VMEM), pl.BlockSpec(memory_space=pl.ANY)],
        out_specs=pl.BlockSpec(memory_space=pl.ANY),
        scratch_shapes=scratch,
        compiler_params=pltpu.CompilerParams(
            collective_id=0, has_side_effects=True, vmem_limit_bytes=56 * 2**20
        ),
        name="exchange",
    )(ask, atm)


def remap_kernel(count, slots, targets, weight, blocks, out, w_buf, x_buf, w_sem, x_sem):
    live = count[0]
    steps = (live + GROUP - 1) // GROUP

    def copies(step, at):
        first = step * GROUP
        yield pltpu.make_async_copy(weight.at[pl.ds(first, GROUP)], w_buf.at[at], w_sem.at[at])
        for i in range(GROUP):
            yield pltpu.make_async_copy(blocks.at[slots[first + i]], x_buf.at[at, i], x_sem.at[at, i])

    def fetch(step):
        @pl.when(step < steps)
        def _():
            for copy in copies(step, lax.rem(step, DEPTH)):
                copy.start()

    out[...] = jnp.zeros_like(out)
    for step in range(DEPTH - 1):
        fetch(step)

    def body(step, carry):
        at = lax.rem(step, DEPTH)
        fetch(step + DEPTH - 1)
        for copy in copies(step, at):
            copy.wait()
        for i in range(GROUP):
            tile = step * GROUP + i

            @pl.when(tile < live)
            def _():
                out[targets[tile]] += jnp.dot(
                    w_buf[at, i], x_buf[at, i], preferred_element_type=jnp.float32
                )

        return carry

    lax.fori_loop(0, steps, body, 0)


def remap(count, slots, targets, weight, blocks):
    smem = pl.BlockSpec(memory_space=pltpu.SMEM)
    hbm = pl.BlockSpec(memory_space=pl.ANY)
    dma = pltpu.SemaphoreType.DMA
    return pl.pallas_call(
        remap_kernel,
        out_shape=jax.ShapeDtypeStruct((2, ROWS, CHANNELS), jnp.float32),
        in_specs=[smem, smem, smem, hbm, hbm],
        out_specs=pl.BlockSpec(memory_space=pltpu.VMEM),
        scratch_shapes=[
            pltpu.VMEM((DEPTH, GROUP, ROWS, ROWS), jnp.bfloat16),
            pltpu.VMEM((DEPTH, GROUP, ROWS, CHANNELS), jnp.bfloat16),
            dma((DEPTH,)),
            dma((DEPTH, GROUP)),
        ],
        compiler_params=pltpu.CompilerParams(vmem_limit_bytes=24 * 2**20),
        name="remap",
    )(count, slots, targets, weight, blocks)


def plan(tile_src, atm_pos):
    positions = atm_pos[tile_src]
    owners = positions // BLOCKS
    ordinal = jnp.arange(tile_src.shape[0], dtype=jnp.int32)
    earlier = (owners[:, None] == owners[None, :]) & (ordinal[None, :] < ordinal[:, None])
    rank = jnp.sum(earlier.astype(jnp.int32), axis=1)
    gx, gy = lax.axis_index("gx"), lax.axis_index("gy")
    ox, oy = owners // 16, owners % 16
    distance = {
        "x": (gx // 2 - ox // 2) % RING,
        "z": (gy // 4 - oy // 4) % RING,
        "y": (gy % 4 - oy % 4) % RING,
    }
    slots = slot_of(distance, (gx - ox) % CORES, rank)
    matches = slots[None, :] == jnp.arange(256, dtype=jnp.int32)[:, None]
    ask = jnp.sum(jnp.where(matches, (positions % BLOCKS)[None, :], 0), axis=1)
    return slots, ask.reshape(2, 128)


def with_mask(state, mask):
    wide = jnp.broadcast_to(mask[..., None], state.shape)
    return jnp.concatenate([state, wide], axis=0)


def local(atm_fields, atm_pos, tile_src, tile_tgt, tile_count, tile_weight, ocean_state, land_mask, mixing):
    n_gx, n_gy = lax.axis_size("gx"), lax.axis_size("gy")
    mask_half = land_mask.astype(jnp.bfloat16)
    lat, lon = mask_half.shape
    ring_up = [(i, (i + 1) % n_gx) for i in range(n_gx)]
    ring_down = [(j, i) for i, j in ring_up]
    line_up = [(i, i + 1) for i in range(n_gy - 1)]
    line_down = [(j, i) for i, j in line_up]
    west = lax.ppermute(with_mask(ocean_state[:, -1], mask_half[:, -1]), "gx", ring_up)
    east = lax.ppermute(with_mask(ocean_state[:, 0], mask_half[:, 0]), "gx", ring_down)
    top = with_mask(ocean_state[-1], mask_half[-1])
    south = lax.ppermute(top, "gy", line_up)
    north = lax.ppermute(with_mask(ocean_state[0], mask_half[0]), "gy", line_down)
    flipped = with_mask(ocean_state[-1, ::-1], mask_half[-1, ::-1])
    fold = lax.ppermute(flipped, "gx", [(i, n_gx - 1 - i) for i in range(n_gx)])

    slots, ask = plan(tile_src, atm_pos)
    blocks = exchange(ask, atm_fields.reshape(BLOCKS, ROWS, CHANNELS))
    remapped = remap(tile_count, slots, tile_tgt, tile_weight, blocks.reshape(256, ROWS, CHANNELS))
    forcing = remapped.reshape(lat, lon, CHANNELS)

    north = jnp.where(lax.axis_index("gy") == n_gy - 1, fold, north)
    center = ocean_state.astype(jnp.float32)
    wet = jnp.broadcast_to(mask_half[..., None], ocean_state.shape)

    def around(values, part):
        lead, tail = (lambda v, n: v[:n], lambda v, n: v[n:])
        pick = lead if part == 0 else tail
        w, e = pick(west, lat)[:, None], pick(east, lat)[:, None]
        s, n = pick(south, lon)[None], pick(north, lon)[None]
        return (
            jnp.concatenate([w, values[:, :-1]], axis=1),
            jnp.concatenate([values[:, 1:], e], axis=1),
            jnp.concatenate([s, values[:-1]], axis=0),
            jnp.concatenate([values[1:], n], axis=0),
        )

    diffusion = jnp.zeros_like(center)
    for side_state, side_mask in zip(around(ocean_state, 0), around(wet, 1)):
        diffusion = diffusion + side_mask.astype(jnp.float32) * (side_state.astype(jnp.float32) - center)
    result = wet.astype(jnp.float32) * (center + forcing + mixing * diffusion)
    return result.astype(jnp.bfloat16)


def solution(mesh):
    both = ("gx", "gy")
    in_specs = (
        P(both, None),
        P(),
        P(both),
        P(both),
        P(both),
        P(both, None, None),
        P("gy", "gx", None),
        P("gy", "gx"),
        P(),
    )
    return jax.shard_map(
        local, mesh=mesh, in_specs=in_specs, out_specs=P("gy", "gx", None), check_vma=False
    )
```

```python
import functools

import jax
import jax.numpy as jnp
from jax import lax
from jax.experimental import pallas as pl
from jax.experimental.pallas import tpu as pltpu
from jax.sharding import PartitionSpec as P

MESH = pl.DeviceIdType.MESH
ROWS = 256
CHANNELS = 128
BLOCKS = 24
RING = 4
CORES = 2
CLASSES = ((0, 96, "xyz"), (96, 80, "yzx"), (176, 80, "zxy"))
FAR = (1, 3, 2)
GROUP = 8
DEPTH = 4
EXCHANGE_VMEM = 56 * 2**20


def peer(axis, offset, flip=0):
    gx, gy = lax.axis_index("gx"), lax.axis_index("gy")
    x, core, z, y = gx // 2, gx % 2, gy // 4, gy % 4
    if axis == "x":
        x = (x + offset) % RING
    if axis == "y":
        y = (y + offset) % RING
    if axis == "z":
        z = (z + offset) % RING
    core = (core + flip) % CORES
    return (x * 2 + core, z * 4 + y)


def where_from(position):
    gx, gy = lax.axis_index("gx"), lax.axis_index("gy")
    owner = lax.shift_right_logical(position * 2731, 16)
    ox, oy = lax.shift_right_logical(owner, 4), owner & 15
    dx = (gx // 2 - lax.shift_right_logical(ox, 1)) & 3
    dk = (gx - ox) & 1
    dz = (gy // 4 - lax.shift_right_logical(oy, 2)) & 3
    dy = (gy - oy) & 3
    return relative({"x": dx, "z": dz, "y": dy}, dk), position - owner * BLOCKS


def relative(distance, core):
    return ((distance["x"] * CORES + core) * RING + distance["z"]) * RING + distance["y"]


def exchange_kernel(positions, sources, atm, state, mask, final, west, east, south, north, masks, firsts, *scratch):
    kept, gathered, sent, relayed, first, second = (scratch[3 * i : 3 * i + 3] for i in range(6))
    (ask, table, ask_sem, ask_s, ask_r, mid_s, mid_r, smem_sem, own_sem, ag_s, ag_r,
     p2_s, p2_r, p3_s, p3_r, edge_s, edge_r) = scratch[18:]

    barrier = pltpu.get_barrier_semaphore()
    neighbours = [(a, o, f) for a in "xyz" for o in (1, 2, 3) for f in (0, 1)] + [("x", 0, 1)]
    for axis, offset, flip in neighbours:
        pl.semaphore_signal(barrier, 1, device_id=peer(axis, offset, flip), device_id_type=MESH)
    gx, gy = lax.axis_index("gx"), lax.axis_index("gy")
    n_gx, n_gy = lax.axis_size("gx"), lax.axis_size("gy")
    is_top = gy == n_gy - 1
    before, after = ((gx + n_gx - 1) % n_gx, gy), ((gx + 1) % n_gx, gy)
    above = (jnp.where(is_top, n_gx - 1 - gx, gx), jnp.where(is_top, gy, gy + 1))
    below = (gx, gy - 1)
    has_below = gy > 0
    for target in (before, after, above):
        pl.semaphore_signal(barrier, 1, device_id=target, device_id_type=MESH)

    @pl.when(has_below)
    def _():
        pl.semaphore_signal(barrier, 1, device_id=below, device_id_type=MESH)

    lane_of = lax.broadcasted_iota(jnp.int32, (1, 128), 1)
    zero = jnp.zeros((1, 128), jnp.int32)

    def claim(step, carry):
        count, ask0, ask1, leader = carry
        for i in range(8):
            tile = step * 8 + i
            lane, block = where_from(positions[sources[tile]])
            mine = lane_of == lane
            free = mine & (count == 0)
            ask0 = jnp.where(free, block, ask0)
            leader = jnp.where(free, tile, leader)
            ask1 = jnp.where(mine, jnp.where(free, ask1, block), ask1)
            count = jnp.where(mine, 1, count)
        return count, ask0, ask1, leader

    _, ask0, ask1, leader = lax.fori_loop(0, sources.shape[0] // 8, claim, (zero, zero, zero, zero))
    ask[0:1] = ask0
    ask[1:2] = ask1
    firsts[...] = leader

    pl.semaphore_wait(barrier, len(neighbours) + 3 + jnp.where(has_below, 1, 0))

    def copier(src, dst, send, recv, target):
        return pltpu.make_async_remote_copy(
            src_ref=src, dst_ref=dst, send_sem=send, recv_sem=recv, device_id=target, device_id_type=MESH
        )

    def remote(*parts):
        copy = copier(*parts)
        copy.start()
        return copy

    half = BLOCKS // 2
    low, high = pl.ds(0, half), pl.ds(half, half)

    def direct(c, i, offset, part):
        start, size, order = CLASSES[c]
        return remote(
            atm.at[part, pl.ds(start, size)], gathered[c].at[offset - 1, part],
            ag_s.at[c, i], ag_r.at[c, i], peer(order[0], offset),
        )

    def forward(c, i, origin, part):
        return remote(
            gathered[c].at[origin - 1, part], gathered[c].at[1, part],
            ag_s.at[c, i], ag_r.at[c, i], peer(CLASSES[c][2][0], origin),
        )

    rings = [[direct(c, 0, 1, low), direct(c, 1, 3, high)] for c in range(3)]
    owns = []
    for c, (start, size, _) in enumerate(CLASSES):
        own = pltpu.make_async_copy(atm.at[:, pl.ds(start, size)], kept[c], own_sem.at[c])
        own.start()
        owns.append(own)

    def edges(side, slot, target, src, dst):
        return (
            copier(src, dst, edge_s.at[0, side], edge_r.at[0, slot], target),
            copier(mask, masks.at[slot], edge_s.at[1, side], edge_r.at[1, slot], target),
        )

    last = state.shape[0] - 1
    wide = state.shape[1]
    to_before = edges(0, 1, before, state.at[:, pl.ds(0, 8)], east)
    to_after = edges(1, 0, after, state.at[:, pl.ds(wide - 8, 8)], west)
    to_below = edges(2, 3, below, state.at[0], north)
    to_fold = edges(3, 3, above, state.at[last], north)
    to_above = edges(3, 2, above, state.at[last], south)
    for copy in to_before + to_after:
        copy.start()
    for case, group in ((has_below, to_below), (is_top, to_fold), (jnp.logical_not(is_top), to_above)):

        @pl.when(case)
        def _():
            for copy in group:
                copy.start()

    asks, mids, p3s = [], [], []
    for c, (_, _, order) in enumerate(CLASSES):
        local = pltpu.make_async_copy(ask, first[c].at[0], ask_sem.at[c])
        local.start()
        asks.append([local])
        for lane in range(1, RING * CORES):
            o3, flip = lane // CORES, lane % CORES
            asks[c].append(
                remote(ask, first[c].at[lane], ask_s.at[c, lane], ask_r.at[c, lane], peer(order[2], -o3, flip))
            )
    for c in range(3):
        rings[c] += [direct(c, 2, 1, high), direct(c, 3, 3, low)]
    for c, (_, _, order) in enumerate(CLASSES):
        for copy in asks[c]:
            copy.wait()
        mids.append(
            [remote(first[c], second[c].at[o], mid_s.at[c, o], mid_r.at[c, o], peer(order[1], -o)) for o in FAR]
        )
        keep = pltpu.make_async_copy(first[c], table.at[c, 0], smem_sem.at[c, 0])
        keep.start()
        mids[c].append(keep)
    for c in range(3):
        for copy in rings[c][:2]:
            copy.wait()
        rings[c] = rings[c][2:] + [forward(c, 4, 1, low), forward(c, 5, 3, high)]
    keeps = []
    for c in range(3):
        for copy in mids[c]:
            copy.wait()
        for o in FAR:
            keep = pltpu.make_async_copy(second[c].at[o], table.at[c, o], smem_sem.at[c, o])
            keep.start()
            keeps.append(keep)
    for keep in keeps:
        keep.wait()

    def pack(c, o2, origins):
        order = CLASSES[c][2]

        def body(lane, carry):
            o3, flip = lane // CORES, lane % CORES
            for o1 in origins:
                for rank in range(2):
                    at = relative({order[0]: o1, order[1]: o2, order[2]: o3}, flip)
                    which = table[c, o2, lane, rank, at]
                    sent[c][o2, o1, lane, rank] = kept[c][which] if o1 == 0 else gathered[c][o1 - 1, which]
            return carry

        lax.fori_loop(0, RING * CORES, body, 0)

    def send2(c, o2, origins):
        order = CLASSES[c][2]
        part = pl.ds(origins[0], len(origins))
        i = 0 if origins[0] == 0 else 1
        return remote(
            sent[c].at[o2, part], relayed[c].at[o2, part], p2_s.at[c, o2, i], p2_r.at[c, o2, i],
            peer(order[1], o2),
        )

    def send3(c, o2):
        start, size, order = CLASSES[c]
        source = sent[c] if o2 == 0 else relayed[c]
        for lane in range(RING * CORES):
            o3, flip = lane // CORES, lane % CORES
            at = {order[0]: slice(None), order[1]: o2, order[2]: o3}
            dst = final.at[at["x"], flip, at["z"], at["y"], :, pl.ds(start, size)]
            src = source.at[o2, :, lane]
            if lane == 0:
                copy = pltpu.make_async_copy(src, dst, p3_s.at[c, o2, 0])
                copy.start()
                p3s.append(copy)
            else:
                p3s.append(
                    remote(src, dst, p3_s.at[c, o2, lane], p3_r.at[c, o2, lane], peer(order[2], o3, flip))
                )

    pending = {(c, o2): [] for c in range(3) for o2 in FAR}
    near, rest = (0,), (1, 2, 3)
    for owner in owns:
        owner.wait()
    last_step = None
    for origins in (near, rest):
        if origins is rest:
            for c in range(3):
                for copy in rings[c]:
                    copy.wait()
        for o2 in FAR:
            for c in range(3):
                pack(c, o2, origins)
                if last_step is not None:
                    pending[last_step[:2]].append(send2(*last_step))
                last_step = (c, o2, origins)
    for c in range(3):
        pack(c, 0, near + rest)
        if c == 0:
            pending[last_step[:2]].append(send2(*last_step))
        else:
            send3(c - 1, 0)
    for o2 in FAR:
        for c in range(3):
            for copy in pending[c, o2]:
                copy.wait()
            send3(c, o2)
            if (c, o2) == (0, 1):
                send3(2, 0)
    for copy in p3s:
        copy.wait()
    for copy in edges(0, 0, before, state.at[:, pl.ds(0, 8)], west) + edges(1, 1, after, state.at[:, pl.ds(0, 8)], east):
        copy.wait()
    for copy in edges(3, 3, above, state.at[last], north):
        copy.wait()

    @pl.when(has_below)
    def _():
        for copy in edges(2, 2, below, state.at[0], south):
            copy.wait()


def exchange(positions, sources, atm, state, mask):
    dma = pltpu.SemaphoreType.DMA
    tables = RING * CORES
    scratch = [pltpu.VMEM((BLOCKS, size, CHANNELS), jnp.bfloat16) for _, size, _ in CLASSES]
    scratch += [pltpu.VMEM((RING - 1, BLOCKS, size, CHANNELS), jnp.bfloat16) for _, size, _ in CLASSES]
    for _ in range(2):
        scratch += [
            pltpu.VMEM((RING, RING, tables, 2, size, CHANNELS), jnp.bfloat16) for _, size, _ in CLASSES
        ]
    scratch += [pltpu.VMEM((tables, 2, 128), jnp.int32) for _ in CLASSES]
    scratch += [pltpu.VMEM((RING, tables, 2, 128), jnp.int32) for _ in CLASSES]
    scratch += [
        pltpu.VMEM((2, 128), jnp.int32),
        pltpu.SMEM((3, RING, tables, 2, 128), jnp.int32),
        dma((3,)),
        dma((3, tables)),
        dma((3, tables)),
        dma((3, RING)),
        dma((3, RING)),
        dma((3, RING)),
        dma((3,)),
        dma((3, 6)),
        dma((3, 6)),
        dma((3, RING, 2)),
        dma((3, RING, 2)),
        dma((3, RING, tables)),
        dma((3, RING, tables)),
        dma((2, 4)),
        dma((2, 4)),
    ]
    lat, lon = mask.shape
    smem = pl.BlockSpec(memory_space=pltpu.SMEM)
    vmem = pl.BlockSpec(memory_space=pltpu.VMEM)
    free = pl.BlockSpec(memory_space=pl.ANY)
    side = jax.ShapeDtypeStruct((lat, 8, CHANNELS), jnp.bfloat16)
    row = jax.ShapeDtypeStruct((lon, CHANNELS), jnp.bfloat16)
    return pl.pallas_call(
        exchange_kernel,
        out_shape=(
            jax.ShapeDtypeStruct((RING, CORES, RING, RING, 2, ROWS, CHANNELS), jnp.bfloat16),
            side,
            side,
            row,
            row,
            jax.ShapeDtypeStruct((4, lat, lon), jnp.int32),
            jax.ShapeDtypeStruct((1, 128), jnp.int32),
        ),
        in_specs=[smem, smem, free, vmem, vmem],
        out_specs=(free, vmem, vmem, vmem, vmem, vmem, vmem),
        scratch_shapes=scratch,
        compiler_params=pltpu.CompilerParams(
            collective_id=0, has_side_effects=True, vmem_limit_bytes=EXCHANGE_VMEM
        ),
        name="exchange",
    )(positions, sources, atm, state, mask)


def remap_kernel(
    count, positions, sources, firsts, targets, weight, blocks, state, mask, mixing,
    west, east, south, north, masks, out, w_buf, x_buf, total, base, wet, w_sem, x_sem,
):
    live = count[0]
    steps = (live + GROUP - 1) // GROUP

    def slot_of(tile):
        lane, _ = where_from(positions[sources[tile]])
        return lane * 2 + jnp.where(firsts[0, lane] == tile, 0, 1)

    def copies(step, at, started=False):
        first = step * GROUP
        yield pltpu.make_async_copy(weight.at[pl.ds(first, GROUP)], w_buf.at[at], w_sem.at[at])
        for i in range(GROUP):
            slot = slot_of(first + i) if started else 0
            yield pltpu.make_async_copy(blocks.at[slot], x_buf.at[at, i], x_sem.at[at, i])

    def fetch(step):
        @pl.when(step < steps)
        def _():
            for copy in copies(step, lax.rem(step, DEPTH), True):
                copy.start()

    for step in range(DEPTH - 1):
        fetch(step)
    total[...] = jnp.zeros_like(total)
    stencil(state, mask, mixing, west, east, south, north, masks, base, wet)

    def body(step, carry):
        at = lax.rem(step, DEPTH)
        fetch(step + DEPTH - 1)
        for copy in copies(step, at):
            copy.wait()
        zero = jnp.zeros((ROWS, CHANNELS), jnp.bfloat16)
        right = []
        for i in range(GROUP):
            tile = step * GROUP + i
            target = jnp.where(tile < live, targets[tile], 2)
            x = x_buf[at, i]
            right.append(
                jnp.concatenate([jnp.where(target == b, x, zero) for b in range(2)], axis=1)
            )
        left = jnp.concatenate([w_buf[at, i] for i in range(GROUP)], axis=1)
        total[...] += jnp.dot(
            left, jnp.concatenate(right, axis=0), preferred_element_type=jnp.float32
        )
        return carry

    lax.fori_loop(0, steps, body, 0)
    lats, lons, _ = state.shape
    for i in range(lats):
        row = i * lons % ROWS
        b = i * lons // ROWS
        forcing = total[row : row + lons, b * CHANNELS : (b + 1) * CHANNELS]
        out[i] = (base[i] + wet[i] * forcing).astype(out.dtype)


def stencil(state, mask, mixing, west, east, south, north, masks, base, wet):
    gy, n_gy = lax.axis_index("gy"), lax.axis_size("gy")
    lats, lons, channels = state.shape
    shape = (lons, channels)

    def columns(part):
        turned = jnp.transpose(part.astype(jnp.float32))
        return [jnp.broadcast_to(turned[:, i : i + 1], shape) for i in range(part.shape[0])]

    lon = lax.broadcasted_iota(jnp.int32, shape, 0)
    reverse = jnp.where(
        lax.broadcasted_iota(jnp.int32, (lons, lons), 0) + lax.broadcasted_iota(jnp.int32, (lons, lons), 1)
        == lons - 1,
        1.0,
        0.0,
    )

    def flip(part):
        return jnp.dot(
            reverse, part, preferred_element_type=jnp.float32, precision=lax.Precision.HIGHEST
        )

    is_top = gy == n_gy - 1
    wets = columns(mask[...])
    west_wets, east_wets = columns(masks[0]), columns(masks[1])
    south_wet = jnp.where(gy == 0, 0.0, columns(masks[2])[lats - 1])
    from_north = columns(masks[3])
    north_wet = jnp.where(is_top, flip(from_north[lats - 1]), from_north[0])
    south_state = jnp.where(gy == 0, 0.0, south[...].astype(jnp.float32))
    north_plain = north[...].astype(jnp.float32)
    north_state = jnp.where(is_top, flip(north_plain), north_plain)
    states = [state[i].astype(jnp.float32) for i in range(lats)]
    scale = mixing[...]
    for i in range(lats):
        center = states[i]
        from_west = jnp.broadcast_to(west[i].astype(jnp.float32)[-1:], shape)
        from_east = jnp.broadcast_to(east[i].astype(jnp.float32)[:1], shape)
        sides = (
            (
                jnp.where(lon == 0, from_west, pltpu.roll(center, 1, 0)),
                jnp.where(lon == 0, pltpu.roll(west_wets[i], 1, 0), pltpu.roll(wets[i], 1, 0)),
            ),
            (
                jnp.where(lon == lons - 1, from_east, pltpu.roll(center, lons - 1, 0)),
                jnp.where(
                    lon == lons - 1, pltpu.roll(east_wets[i], lons - 1, 0), pltpu.roll(wets[i], lons - 1, 0)
                ),
            ),
            (south_state, south_wet) if i == 0 else (states[i - 1], wets[i - 1]),
            (north_state, north_wet) if i == lats - 1 else (states[i + 1], wets[i + 1]),
        )
        diffusion = jnp.zeros_like(center)
        for side_state, side_wet in sides:
            diffusion = diffusion + side_wet * (side_state - center)
        wet[i] = wets[i]
        base[i] = wets[i] * (center + scale * diffusion)


def remap(count, positions, sources, firsts, targets, weight, blocks, state, mask, mixing, halo):
    smem = pl.BlockSpec(memory_space=pltpu.SMEM)
    vmem = pl.BlockSpec(memory_space=pltpu.VMEM)
    hbm = pl.BlockSpec(memory_space=pl.ANY)
    dma = pltpu.SemaphoreType.DMA
    return pl.pallas_call(
        remap_kernel,
        out_shape=jax.ShapeDtypeStruct(state.shape, state.dtype),
        in_specs=[smem, smem, smem, smem, smem, hbm, hbm] + [vmem] * 8,
        out_specs=vmem,
        scratch_shapes=[
            pltpu.VMEM((DEPTH, GROUP, ROWS, ROWS), jnp.bfloat16),
            pltpu.VMEM((DEPTH, GROUP, ROWS, CHANNELS), jnp.bfloat16),
            pltpu.VMEM((ROWS, 2 * CHANNELS), jnp.float32),
            pltpu.VMEM(state.shape, jnp.float32),
            pltpu.VMEM(state.shape, jnp.float32),
            dma((DEPTH,)),
            dma((DEPTH, GROUP)),
        ],
        compiler_params=pltpu.CompilerParams(vmem_limit_bytes=56 * 2**20),
        name="remap",
    )(count, positions, sources, firsts, targets, weight, blocks, state, mask, mixing, *halo)


def local(atm_fields, atm_pos, tile_src, tile_tgt, tile_count, tile_weight, ocean_state, land_mask, mixing):
    blocks, west, east, south, north, masks, firsts = exchange(
        atm_pos, tile_src, atm_fields.reshape(BLOCKS, ROWS, CHANNELS), ocean_state, land_mask
    )
    return remap(
        tile_count,
        atm_pos,
        tile_src,
        firsts,
        tile_tgt,
        tile_weight,
        blocks.reshape(256, ROWS, CHANNELS),
        ocean_state,
        land_mask,
        mixing.reshape(1, CHANNELS),
        (west, east, south, north, masks),
    )


def solution(mesh):
    both = ("gx", "gy")
    in_specs = (
        P(both, None),
        P(),
        P(both),
        P(both),
        P(both),
        P(both, None, None),
        P("gy", "gx", None),
        P("gy", "gx"),
        P(),
    )
    return jax.shard_map(
        local, mesh=mesh, in_specs=in_specs, out_specs=P("gy", "gx", None), check_vma=False
    )
```

```python
import functools

import jax
import jax.numpy as jnp
from jax import lax
from jax.experimental import pallas as pl
from jax.experimental.pallas import tpu as pltpu
from jax.sharding import PartitionSpec as P

MESH = pl.DeviceIdType.MESH
ROWS = 256
CHANNELS = 128
BLOCKS = 24
RING = 4
CORES = 2
CLASSES = ((0, 96, "xyz"), (96, 80, "yzx"), (176, 80, "zxy"))
FAR = (1, 3, 2)
GROUP = 8
LIST = 48
NOBODY = 31
DEPTH = 4
EXCHANGE_VMEM = 56 * 2**20


def peer(axis, offset, flip=0):
    gx, gy = lax.axis_index("gx"), lax.axis_index("gy")
    x, core, z, y = gx // 2, gx % 2, gy // 4, gy % 4
    if axis == "x":
        x = (x + offset) % RING
    if axis == "y":
        y = (y + offset) % RING
    if axis == "z":
        z = (z + offset) % RING
    core = (core + flip) % CORES
    return (x * 2 + core, z * 4 + y)


def where_from(position):
    gx, gy = lax.axis_index("gx"), lax.axis_index("gy")
    owner = lax.shift_right_logical(position * 2731, 16)
    ox, oy = lax.shift_right_logical(owner, 4), owner & 15
    dx = (gx // 2 - lax.shift_right_logical(ox, 1)) & 3
    dk = (gx - ox) & 1
    dz = (gy // 4 - lax.shift_right_logical(oy, 2)) & 3
    dy = (gy - oy) & 3
    return relative({"x": dx, "z": dz, "y": dy}, dk), position - owner * BLOCKS


def relative(distance, core):
    return ((distance["x"] * CORES + core) * RING + distance["z"]) * RING + distance["y"]


def exchange_kernel(positions, sources, atm, state, mask, final, west, east, south, north, masks, firsts, *scratch):
    kept, gathered, sent, relayed, first, second = (scratch[3 * i : 3 * i + 3] for i in range(6))
    (ask, table, ask_sem, ask_s, ask_r, mid_s, mid_r, smem_sem, own_sem, ag_s, ag_r,
     p2_s, p2_r, p3_s, p3_r, edge_s, edge_r) = scratch[18:]

    barrier = pltpu.get_barrier_semaphore()
    neighbours = [(a, o, f) for a in "xyz" for o in (1, 2, 3) for f in (0, 1)] + [("x", 0, 1)]
    for axis, offset, flip in neighbours:
        pl.semaphore_signal(barrier, 1, device_id=peer(axis, offset, flip), device_id_type=MESH)
    gx, gy = lax.axis_index("gx"), lax.axis_index("gy")
    n_gx, n_gy = lax.axis_size("gx"), lax.axis_size("gy")
    is_top = gy == n_gy - 1
    before, after = ((gx + n_gx - 1) % n_gx, gy), ((gx + 1) % n_gx, gy)
    above = (jnp.where(is_top, n_gx - 1 - gx, gx), jnp.where(is_top, gy, gy + 1))
    below = (gx, gy - 1)
    has_below = gy > 0
    for target in (before, after, above):
        pl.semaphore_signal(barrier, 1, device_id=target, device_id_type=MESH)

    @pl.when(has_below)
    def _():
        pl.semaphore_signal(barrier, 1, device_id=below, device_id_type=MESH)

    lane_of = lax.broadcasted_iota(jnp.int32, (1, 128), 1)
    zero = jnp.zeros((1, 128), jnp.int32)

    def claim(step, carry):
        count, ask0, ask1, leader = carry
        for i in range(8):
            tile = step * 8 + i
            lane, block = where_from(positions[sources[tile]])
            mine = lane_of == lane
            free = mine & (count == 0)
            ask0 = jnp.where(free, block, ask0)
            leader = jnp.where(free, tile, leader)
            ask1 = jnp.where(mine, jnp.where(free, ask1, block), ask1)
            count = jnp.where(mine, 1, count)
        return count, ask0, ask1, leader

    _, ask0, ask1, leader = lax.fori_loop(0, sources.shape[0] // 8, claim, (zero, zero, zero, zero))
    ask[0:1] = ask0
    ask[1:2] = ask1
    firsts[...] = leader

    pl.semaphore_wait(barrier, len(neighbours) + 3 + jnp.where(has_below, 1, 0))

    def copier(src, dst, send, recv, target):
        return pltpu.make_async_remote_copy(
            src_ref=src, dst_ref=dst, send_sem=send, recv_sem=recv, device_id=target, device_id_type=MESH
        )

    def remote(*parts):
        copy = copier(*parts)
        copy.start()
        return copy

    half = BLOCKS // 2
    low, high = pl.ds(0, half), pl.ds(half, half)

    def direct(c, i, offset, part):
        start, size, order = CLASSES[c]
        return remote(
            atm.at[part, pl.ds(start, size)], gathered[c].at[offset - 1, part],
            ag_s.at[c, i], ag_r.at[c, i], peer(order[0], offset),
        )

    def forward(c, i, origin, part):
        return remote(
            gathered[c].at[origin - 1, part], gathered[c].at[1, part],
            ag_s.at[c, i], ag_r.at[c, i], peer(CLASSES[c][2][0], origin),
        )

    rings = [[direct(c, 0, 1, low), direct(c, 1, 3, high)] for c in range(3)]
    owns = []
    for c, (start, size, _) in enumerate(CLASSES):
        own = pltpu.make_async_copy(atm.at[:, pl.ds(start, size)], kept[c], own_sem.at[c])
        own.start()
        owns.append(own)

    def edges(side, slot, target, src, dst):
        return (
            copier(src, dst, edge_s.at[0, side], edge_r.at[0, slot], target),
            copier(mask, masks.at[slot], edge_s.at[1, side], edge_r.at[1, slot], target),
        )

    last = state.shape[0] - 1
    wide = state.shape[1]
    to_before = edges(0, 1, before, state.at[:, pl.ds(0, 8)], east)
    to_after = edges(1, 0, after, state.at[:, pl.ds(wide - 8, 8)], west)
    to_below = edges(2, 3, below, state.at[0], north)
    to_fold = edges(3, 3, above, state.at[last], north)
    to_above = edges(3, 2, above, state.at[last], south)
    for copy in to_before + to_after:
        copy.start()
    for case, group in ((has_below, to_below), (is_top, to_fold), (jnp.logical_not(is_top), to_above)):

        @pl.when(case)
        def _():
            for copy in group:
                copy.start()

    asks, mids, p3s = [], [], []
    for c, (_, _, order) in enumerate(CLASSES):
        local = pltpu.make_async_copy(ask, first[c].at[0], ask_sem.at[c])
        local.start()
        asks.append([local])
        for lane in range(1, RING * CORES):
            o3, flip = lane // CORES, lane % CORES
            asks[c].append(
                remote(ask, first[c].at[lane], ask_s.at[c, lane], ask_r.at[c, lane], peer(order[2], -o3, flip))
            )
    for c in range(3):
        rings[c] += [direct(c, 2, 1, high), direct(c, 3, 3, low)]
    for c, (_, _, order) in enumerate(CLASSES):
        for copy in asks[c]:
            copy.wait()
        mids.append(
            [remote(first[c], second[c].at[o], mid_s.at[c, o], mid_r.at[c, o], peer(order[1], -o)) for o in FAR]
        )
        keep = pltpu.make_async_copy(first[c], table.at[c, 0], smem_sem.at[c, 0])
        keep.start()
        mids[c].append(keep)
    for c in range(3):
        for copy in rings[c][:2]:
            copy.wait()
        rings[c] = rings[c][2:] + [forward(c, 4, 1, low), forward(c, 5, 3, high)]
    keeps = []
    for c in range(3):
        for copy in mids[c]:
            copy.wait()
        for o in FAR:
            keep = pltpu.make_async_copy(second[c].at[o], table.at[c, o], smem_sem.at[c, o])
            keep.start()
            keeps.append(keep)
    for keep in keeps:
        keep.wait()

    def pack(c, o2, origins):
        order = CLASSES[c][2]

        def body(lane, carry):
            o3, flip = lane // CORES, lane % CORES
            for o1 in origins:
                for rank in range(2):
                    at = relative({order[0]: o1, order[1]: o2, order[2]: o3}, flip)
                    which = table[c, o2, lane, rank, at]
                    sent[c][o2, o1, lane, rank] = kept[c][which] if o1 == 0 else gathered[c][o1 - 1, which]
            return carry

        lax.fori_loop(0, RING * CORES, body, 0)

    def send2(c, o2, origins):
        order = CLASSES[c][2]
        part = pl.ds(origins[0], len(origins))
        i = 0 if origins[0] == 0 else 1
        return remote(
            sent[c].at[o2, part], relayed[c].at[o2, part], p2_s.at[c, o2, i], p2_r.at[c, o2, i],
            peer(order[1], o2),
        )

    def send3(c, o2):
        start, size, order = CLASSES[c]
        source = sent[c] if o2 == 0 else relayed[c]
        for lane in range(RING * CORES):
            o3, flip = lane // CORES, lane % CORES
            at = {order[0]: slice(None), order[1]: o2, order[2]: o3}
            dst = final.at[at["x"], flip, at["z"], at["y"], :, pl.ds(start, size)]
            src = source.at[o2, :, lane]
            if lane == 0:
                copy = pltpu.make_async_copy(src, dst, p3_s.at[c, o2, 0])
                copy.start()
                p3s.append(copy)
            else:
                p3s.append(
                    remote(src, dst, p3_s.at[c, o2, lane], p3_r.at[c, o2, lane], peer(order[2], o3, flip))
                )

    pending = {(c, o2): [] for c in range(3) for o2 in FAR}
    near, rest = (0,), (1, 2, 3)
    for owner in owns:
        owner.wait()
    last_step = None
    for origins in (near, rest):
        if origins is rest:
            for c in range(3):
                for copy in rings[c]:
                    copy.wait()
        for o2 in FAR:
            for c in range(3):
                pack(c, o2, origins)
                if last_step is not None:
                    pending[last_step[:2]].append(send2(*last_step))
                last_step = (c, o2, origins)
    for c in range(3):
        pack(c, 0, near + rest)
        if c == 0:
            pending[last_step[:2]].append(send2(*last_step))
        else:
            send3(c - 1, 0)
    for o2 in FAR:
        for c in range(3):
            for copy in pending[c, o2]:
                copy.wait()
            send3(c, o2)
            if (c, o2) == (0, 1):
                send3(2, 0)
    for copy in p3s:
        copy.wait()
    for copy in edges(0, 0, before, state.at[:, pl.ds(0, 8)], west) + edges(1, 1, after, state.at[:, pl.ds(0, 8)], east):
        copy.wait()
    for copy in edges(3, 3, above, state.at[last], north):
        copy.wait()

    @pl.when(has_below)
    def _():
        for copy in edges(2, 2, below, state.at[0], south):
            copy.wait()


def exchange(positions, sources, atm, state, mask):
    dma = pltpu.SemaphoreType.DMA
    tables = RING * CORES
    scratch = [pltpu.VMEM((BLOCKS, size, CHANNELS), jnp.bfloat16) for _, size, _ in CLASSES]
    scratch += [pltpu.VMEM((RING - 1, BLOCKS, size, CHANNELS), jnp.bfloat16) for _, size, _ in CLASSES]
    for _ in range(2):
        scratch += [
            pltpu.VMEM((RING, RING, tables, 2, size, CHANNELS), jnp.bfloat16) for _, size, _ in CLASSES
        ]
    scratch += [pltpu.VMEM((tables, 2, 128), jnp.int32) for _ in CLASSES]
    scratch += [pltpu.VMEM((RING, tables, 2, 128), jnp.int32) for _ in CLASSES]
    scratch += [
        pltpu.VMEM((2, 128), jnp.int32),
        pltpu.SMEM((3, RING, tables, 2, 128), jnp.int32),
        dma((3,)),
        dma((3, tables)),
        dma((3, tables)),
        dma((3, RING)),
        dma((3, RING)),
        dma((3, RING)),
        dma((3,)),
        dma((3, 6)),
        dma((3, 6)),
        dma((3, RING, 2)),
        dma((3, RING, 2)),
        dma((3, RING, tables)),
        dma((3, RING, tables)),
        dma((2, 4)),
        dma((2, 4)),
    ]
    lat, lon = mask.shape
    smem = pl.BlockSpec(memory_space=pltpu.SMEM)
    vmem = pl.BlockSpec(memory_space=pltpu.VMEM)
    free = pl.BlockSpec(memory_space=pl.ANY)
    side = jax.ShapeDtypeStruct((lat, 8, CHANNELS), jnp.bfloat16)
    row = jax.ShapeDtypeStruct((lon, CHANNELS), jnp.bfloat16)
    return pl.pallas_call(
        exchange_kernel,
        out_shape=(
            jax.ShapeDtypeStruct((RING, CORES, RING, RING, 2, ROWS, CHANNELS), jnp.bfloat16),
            side,
            side,
            row,
            row,
            jax.ShapeDtypeStruct((4, lat, lon), jnp.int32),
            jax.ShapeDtypeStruct((1, 128), jnp.int32),
        ),
        in_specs=[smem, smem, free, vmem, vmem],
        out_specs=(free, vmem, vmem, vmem, vmem, vmem, vmem),
        scratch_shapes=scratch,
        compiler_params=pltpu.CompilerParams(
            collective_id=0, has_side_effects=True, vmem_limit_bytes=EXCHANGE_VMEM
        ),
        name="exchange",
    )(positions, sources, atm, state, mask)


def lean_kernel(
    count, positions, sources, atm, state, mask,
    final, west, east, south, north, masks, firsts, flag, *scratch
):
    kept, gathered, sent, out3, first = (scratch[3 * i : 3 * i + 3] for i in range(5))
    relayed = [scratch[15 + 3 * c : 18 + 3 * c] for c in range(3)]
    (ask, needs, spots, lists, heard, over1, over2, over3, over1_in, over2_in, over3_in,
     table, spot_table, list_table, ask_sem, ask_s, ask_r, list_s, list_r, smem_sem, own_sem,
     ag_s, ag_r, p2_s, p2_r, p3_s, p3_r, edge_s, edge_r, over_s, over_r) = scratch[24:]

    barrier = pltpu.get_barrier_semaphore()
    neighbours = [(a, o, f) for a in "xyz" for o in (1, 2, 3) for f in (0, 1)] + [("x", 0, 1)]
    for axis, offset, flip in neighbours:
        pl.semaphore_signal(barrier, 1, device_id=peer(axis, offset, flip), device_id_type=MESH)
    gx, gy = lax.axis_index("gx"), lax.axis_index("gy")
    n_gx, n_gy = lax.axis_size("gx"), lax.axis_size("gy")
    is_top = gy == n_gy - 1
    before, after = ((gx + n_gx - 1) % n_gx, gy), ((gx + 1) % n_gx, gy)
    above = (jnp.where(is_top, n_gx - 1 - gx, gx), jnp.where(is_top, gy, gy + 1))
    below = (gx, gy - 1)
    has_below = gy > 0
    for target in (before, after, above):
        pl.semaphore_signal(barrier, 1, device_id=target, device_id_type=MESH)

    @pl.when(has_below)
    def _():
        pl.semaphore_signal(barrier, 1, device_id=below, device_id_type=MESH)

    lane_of = lax.broadcasted_iota(jnp.int32, (1, 128), 1)
    zero = jnp.zeros((1, 128), jnp.int32)
    live = count[0]

    def claim(step, carry):
        taken, ask0, ask1, leader = carry
        for i in range(8):
            tile = step * 8 + i
            lane, block = where_from(positions[sources[tile]])
            mine = lane_of == jnp.where(tile < live, lane, 128)
            free = mine & (taken == 0)
            ask0 = jnp.where(free, block, ask0)
            leader = jnp.where(free, tile, leader)
            ask1 = jnp.where(mine, jnp.where(free, ask1, block), ask1)
            taken = jnp.where(mine, 1, taken)
        return taken, ask0, ask1, leader

    _, ask0, ask1, leader = lax.fori_loop(
        0, sources.shape[0] // 8, claim, (zero, zero + NOBODY, zero + NOBODY, zero)
    )
    ask[0:1] = ask0
    ask[1:2] = ask1
    firsts[...] = leader
    pl.semaphore_wait(barrier, len(neighbours) + 3 + jnp.where(has_below, 1, 0))

    def copier(src, dst, send, recv, target):
        return pltpu.make_async_remote_copy(
            src_ref=src, dst_ref=dst, send_sem=send, recv_sem=recv, device_id=target, device_id_type=MESH
        )

    def remote(*parts):
        copy = copier(*parts)
        copy.start()
        return copy

    def keep(src, dst, sem):
        copy = pltpu.make_async_copy(src, dst, sem)
        copy.start()
        return copy

    half = BLOCKS // 2
    low, high = pl.ds(0, half), pl.ds(half, half)

    def direct(c, i, offset, part):
        start, size, order = CLASSES[c]
        return remote(
            atm.at[part, pl.ds(start, size)], gathered[c].at[offset, part],
            ag_s.at[c, i], ag_r.at[c, i], peer(order[0], offset),
        )

    def forward(c, i, origin, part):
        return remote(
            gathered[c].at[origin, part], gathered[c].at[2, part],
            ag_s.at[c, i], ag_r.at[c, i], peer(CLASSES[c][2][0], origin),
        )

    rings = [[direct(c, 0, 1, low), direct(c, 1, 3, high)] for c in range(3)]
    owns = []
    for c, (start, size, _) in enumerate(CLASSES):
        owns.append(keep(atm.at[:, pl.ds(start, size)], kept[c], own_sem.at[c, 0]))
        rings[c].append(keep(atm.at[:, pl.ds(start, size)], gathered[c].at[0], own_sem.at[c, 1]))

    def edges(side, slot, target, src, dst):
        return (
            copier(src, dst, edge_s.at[0, side], edge_r.at[0, slot], target),
            copier(mask, masks.at[slot], edge_s.at[1, side], edge_r.at[1, slot], target),
        )

    last = state.shape[0] - 1
    wide = state.shape[1]
    to_before = edges(0, 1, before, state.at[:, pl.ds(0, 8)], east)
    to_after = edges(1, 0, after, state.at[:, pl.ds(wide - 8, 8)], west)
    to_below = edges(2, 3, below, state.at[0], north)
    to_fold = edges(3, 3, above, state.at[last], north)
    to_above = edges(3, 2, above, state.at[last], south)
    for copy in to_before + to_after:
        copy.start()
    for case, group in ((has_below, to_below), (is_top, to_fold), (jnp.logical_not(is_top), to_above)):

        @pl.when(case)
        def _():
            for copy in group:
                copy.start()

    asks = []
    for c, (_, _, order) in enumerate(CLASSES):
        asks.append([keep(ask, first[c].at[0], ask_sem.at[c])])
        for lane in range(1, RING * CORES):
            o3, flip = lane // CORES, lane % CORES
            asks[c].append(
                remote(ask, first[c].at[lane], ask_s.at[c, lane], ask_r.at[c, lane], peer(order[2], -o3, flip))
            )
    for c in range(3):
        rings[c] += [direct(c, 2, 1, high), direct(c, 3, 3, low)]

    def wanted(c, o1, o2, lane, rank):
        order = CLASSES[c][2]
        o3, flip = lane // CORES, lane % CORES
        return table[c, lane, rank, relative({order[0]: o1, order[1]: o2, order[2]: o3}, flip)]

    keeps = []
    for c in range(3):
        for copy in asks[c]:
            copy.wait()
        keeps.append(keep(first[c], table.at[c], smem_sem.at[0, c]))
    needs[...] = jnp.zeros_like(needs)
    for c in range(3):
        keeps[c].wait()

        def mark(lane, seen):
            seen = list(seen)
            for o2 in FAR:
                for o1 in range(RING):
                    for rank in range(2):
                        key = o1 * 32 + wanted(c, o1, o2, lane, rank)
                        seen[o2 - 1] = jnp.where(lane_of == key, 1, seen[o2 - 1])
            return tuple(seen)

        seen = lax.fori_loop(0, RING * CORES, mark, (zero, zero, zero))
        for o2 in FAR:
            row = c * 3 + o2 - 1
            needs[row : row + 1] = jnp.where((lane_of & 31) < BLOCKS, seen[o2 - 1], 0)

    need = needs[...]
    upper = lax.broadcasted_iota(jnp.int32, (128, 128), 0) < lax.broadcasted_iota(jnp.int32, (128, 128), 1)
    spot = jnp.dot(
        need.astype(jnp.float32).astype(jnp.bfloat16),
        jnp.where(upper, 1.0, 0.0).astype(jnp.bfloat16),
        preferred_element_type=jnp.float32,
    ).astype(jnp.int32)
    over1[...] = jnp.where((need > 0) & (spot >= LIST), 1, 0)
    spots[...] = jnp.clip(spot, 0, LIST - 1)
    keys = lax.broadcasted_iota(jnp.int32, (8, 128), 1).astype(jnp.float32).astype(jnp.bfloat16)
    place = lax.broadcasted_iota(jnp.int32, (128, 128), 0)
    for row in range(9):
        mine = (spot[row : row + 1] == place) & (need[row : row + 1] > 0)
        lists[row] = lax.dot_general(
            keys,
            jnp.where(mine, 1.0, 0.0).astype(jnp.bfloat16),
            (((1,), (1,)), ((), ())),
            preferred_element_type=jnp.float32,
        ).astype(jnp.int32)

    def pack3(c, o2, origins):
        def body(lane, carry):
            for o1 in origins:
                for rank in range(2):
                    which = wanted(c, o1, o2, lane, rank) & 31
                    if o2:
                        at = jnp.clip(spot_table[c * 3 + o2 - 1, o1 * 32 + which], 0, LIST - 1)
                        block = relayed[c][o2 - 1][at]
                    elif o1 == 0:
                        block = kept[c][jnp.minimum(which, BLOCKS - 1)]
                    else:
                        block = gathered[c][o1, jnp.minimum(which, BLOCKS - 1)]
                    out3[c][o2, lane, o1, rank] = block
            return carry

        lax.fori_loop(0, RING * CORES, body, 0)

    p3s = []

    def send3(c, o2, origins, part):
        start, size, order = CLASSES[c]
        span = pl.ds(origins[0], len(origins))
        for lane in range(RING * CORES):
            o3, flip = lane // CORES, lane % CORES
            at = {order[0]: span, order[1]: o2, order[2]: o3}
            dst = final.at[at["x"], flip, at["z"], at["y"], :, pl.ds(start, size)]
            src = out3[c].at[o2, lane, span]
            if lane == 0:
                p3s.append(keep(src, dst, p3_s.at[c, part, 0]))
            else:
                p3s.append(
                    remote(src, dst, p3_s.at[c, part, lane], p3_r.at[c, part, lane], peer(order[2], o3, flip))
                )

    near, rest, every = (0,), (1, 2, 3), (0, 1, 2, 3)
    spot_keep = keep(spots, spot_table, smem_sem.at[1, 0])
    for owner in owns:
        owner.wait()
    pack3(0, 0, near)
    tells = []
    for c, (_, _, order) in enumerate(CLASSES):
        for o2 in FAR:
            row = c * 3 + o2 - 1
            tells.append(
                remote(lists.at[row], heard.at[row], list_s.at[row], list_r.at[row], peer(order[1], -o2))
            )
    circle = [(o, f) for o in range(RING) for f in range(CORES) if o or f]
    votes = [
        remote(over1, over1_in.at[i], over_s.at[i], over_r.at[i], peer("x", o, f))
        for i, (o, f) in enumerate(circle)
    ]
    for c in range(3):
        for copy in rings[c][:3]:
            copy.wait()
        rings[c] = rings[c][3:] + [forward(c, 4, 1, low), forward(c, 5, 3, high)]
    pack3(1, 0, near)
    send3(0, 0, near, 4)
    pack3(2, 0, near)
    send3(1, 0, near, 4)
    for row, copy in enumerate(tells):
        copy.wait()
    list_keep = keep(heard, list_table, smem_sem.at[1, 1])
    send3(2, 0, near, 4)
    list_keep.wait()
    spot_keep.wait()
    for c in range(3):
        for copy in rings[c]:
            copy.wait()

    def pack2(c, o2):
        row = c * 3 + o2 - 1

        def body(step, carry):
            for i in range(8):
                slot = step * 8 + i
                key = list_table[row, 0, slot]
                origin = lax.shift_right_logical(key, 5)
                sent[c][o2 - 1, slot] = gathered[c][origin & 3, jnp.minimum(key & 31, BLOCKS - 1)]
            return carry

        lax.fori_loop(0, LIST // 8, body, 0)

    def send2(c, o2):
        return remote(
            sent[c].at[o2 - 1], relayed[c][o2 - 1], p2_s.at[c, o2 - 1], p2_r.at[c, o2 - 1],
            peer(CLASSES[c][2][1], o2),
        )

    steps = [(c, o2) for o2 in FAR for c in range(3)]
    pending = {}
    for i, step in enumerate(steps):
        pack2(*step)
        if i:
            pending[steps[i - 1]] = send2(*steps[i - 1])
    pack3(0, 0, rest)
    pending[steps[-1]] = send2(*steps[-1])
    for copy in votes:
        copy.wait()
    over2[...] = functools.reduce(jnp.maximum, [over1_in[i] for i in range(len(circle))], over1[...])
    pack3(1, 0, rest)
    send3(0, 0, rest, 0)
    pack3(2, 0, rest)
    send3(1, 0, rest, 0)
    votes = [
        remote(over2, over2_in.at[o - 1], over_s.at[7 + o - 1], over_r.at[7 + o - 1], peer("y", o)) for o in FAR
    ]
    send3(2, 0, rest, 0)
    for i, (c, o2) in enumerate(steps):
        pending[c, o2].wait()
        pack3(c, o2, every)
        send3(c, o2, every, o2)
        if i == 2:
            for copy in votes:
                copy.wait()
            over3[...] = functools.reduce(jnp.maximum, [over2_in[k] for k in range(3)], over2[...])
        if i == 3:
            votes = [
                remote(over3, over3_in.at[o - 1], over_s.at[10 + o - 1], over_r.at[10 + o - 1], peer("z", o))
                for o in FAR
            ]
    for copy in votes:
        copy.wait()
    verdict = functools.reduce(jnp.maximum, [over3_in[k] for k in range(3)], over3[...])
    flag[0] = jnp.max(verdict)
    for copy in p3s:
        copy.wait()
    for copy in edges(0, 0, before, state.at[:, pl.ds(0, 8)], west) + edges(1, 1, after, state.at[:, pl.ds(0, 8)], east):
        copy.wait()
    for copy in edges(3, 3, above, state.at[last], north):
        copy.wait()

    @pl.when(has_below)
    def _():
        for copy in edges(2, 2, below, state.at[0], south):
            copy.wait()


def lean_exchange(count, positions, sources, atm, state, mask):
    dma = pltpu.SemaphoreType.DMA
    tables = RING * CORES
    sizes = [size for _, size, _ in CLASSES]
    scratch = [pltpu.VMEM((BLOCKS, size, CHANNELS), jnp.bfloat16) for size in sizes]
    scratch += [pltpu.VMEM((RING, BLOCKS, size, CHANNELS), jnp.bfloat16) for size in sizes]
    scratch += [pltpu.VMEM((3, LIST, size, CHANNELS), jnp.bfloat16) for size in sizes]
    scratch += [pltpu.VMEM((RING, tables, RING, 2, size, CHANNELS), jnp.bfloat16) for size in sizes]
    scratch += [pltpu.VMEM((tables, 2, 128), jnp.int32) for _ in sizes]
    for size in sizes:
        scratch += [pltpu.VMEM((LIST, size, CHANNELS), jnp.bfloat16) for _ in range(3)]
    votes = pltpu.VMEM((16, 128), jnp.int32)
    scratch += [
        pltpu.VMEM((2, 128), jnp.int32),
        votes,
        votes,
        pltpu.VMEM((9, 8, 128), jnp.int32),
        pltpu.VMEM((9, 8, 128), jnp.int32),
        votes,
        votes,
        votes,
        pltpu.VMEM((7, 16, 128), jnp.int32),
        pltpu.VMEM((3, 16, 128), jnp.int32),
        pltpu.VMEM((3, 16, 128), jnp.int32),
        pltpu.SMEM((3, tables, 2, 128), jnp.int32),
        pltpu.SMEM((16, 128), jnp.int32),
        pltpu.SMEM((9, 8, 128), jnp.int32),
        dma((3,)),
        dma((3, tables)),
        dma((3, tables)),
        dma((9,)),
        dma((9,)),
        dma((2, 3)),
        dma((3, 2)),
        dma((3, 6)),
        dma((3, 6)),
        dma((3, 3)),
        dma((3, 3)),
        dma((3, RING + 1, tables)),
        dma((3, RING + 1, tables)),
        dma((2, 4)),
        dma((2, 4)),
        dma((13,)),
        dma((13,)),
    ]
    lat, lon = mask.shape
    smem = pl.BlockSpec(memory_space=pltpu.SMEM)
    vmem = pl.BlockSpec(memory_space=pltpu.VMEM)
    free = pl.BlockSpec(memory_space=pl.ANY)
    side = jax.ShapeDtypeStruct((lat, 8, CHANNELS), jnp.bfloat16)
    row = jax.ShapeDtypeStruct((lon, CHANNELS), jnp.bfloat16)
    return pl.pallas_call(
        lean_kernel,
        out_shape=(
            jax.ShapeDtypeStruct((RING, CORES, RING, RING, 2, ROWS, CHANNELS), jnp.bfloat16),
            side,
            side,
            row,
            row,
            jax.ShapeDtypeStruct((4, lat, lon), jnp.int32),
            jax.ShapeDtypeStruct((1, 128), jnp.int32),
            jax.ShapeDtypeStruct((1,), jnp.int32),
        ),
        in_specs=[smem, smem, smem, free, vmem, vmem],
        out_specs=(free, vmem, vmem, vmem, vmem, vmem, vmem, smem),
        scratch_shapes=scratch,
        compiler_params=pltpu.CompilerParams(
            collective_id=1, has_side_effects=True, vmem_limit_bytes=EXCHANGE_VMEM
        ),
        name="lean_exchange",
    )(count, positions, sources, atm, state, mask)


def remap_kernel(
    count, positions, sources, firsts, targets, weight, blocks, state, mask, mixing,
    west, east, south, north, masks, out, w_buf, x_buf, total, base, wet, w_sem, x_sem,
):
    live = count[0]
    steps = (live + GROUP - 1) // GROUP

    def slot_of(tile):
        lane, _ = where_from(positions[sources[tile]])
        return lane * 2 + jnp.where(firsts[0, lane] == tile, 0, 1)

    def copies(step, at, started=False):
        first = step * GROUP
        yield pltpu.make_async_copy(weight.at[pl.ds(first, GROUP)], w_buf.at[at], w_sem.at[at])
        for i in range(GROUP):
            slot = slot_of(first + i) if started else 0
            yield pltpu.make_async_copy(blocks.at[slot], x_buf.at[at, i], x_sem.at[at, i])

    def fetch(step):
        @pl.when(step < steps)
        def _():
            for copy in copies(step, lax.rem(step, DEPTH), True):
                copy.start()

    for step in range(DEPTH - 1):
        fetch(step)
    total[...] = jnp.zeros_like(total)
    stencil(state, mask, mixing, west, east, south, north, masks, base, wet)

    def body(step, carry):
        at = lax.rem(step, DEPTH)
        fetch(step + DEPTH - 1)
        for copy in copies(step, at):
            copy.wait()
        zero = jnp.zeros((ROWS, CHANNELS), jnp.bfloat16)
        right = []
        for i in range(GROUP):
            tile = step * GROUP + i
            target = jnp.where(tile < live, targets[tile], 2)
            x = x_buf[at, i]
            right.append(
                jnp.concatenate([jnp.where(target == b, x, zero) for b in range(2)], axis=1)
            )
        left = jnp.concatenate([w_buf[at, i] for i in range(GROUP)], axis=1)
        total[...] += jnp.dot(
            left, jnp.concatenate(right, axis=0), preferred_element_type=jnp.float32
        )
        return carry

    lax.fori_loop(0, steps, body, 0)
    lats, lons, _ = state.shape
    for i in range(lats):
        row = i * lons % ROWS
        b = i * lons // ROWS
        forcing = total[row : row + lons, b * CHANNELS : (b + 1) * CHANNELS]
        out[i] = (base[i] + wet[i] * forcing).astype(out.dtype)


def stencil(state, mask, mixing, west, east, south, north, masks, base, wet):
    gy, n_gy = lax.axis_index("gy"), lax.axis_size("gy")
    lats, lons, channels = state.shape
    shape = (lons, channels)

    def columns(part):
        turned = jnp.transpose(part.astype(jnp.float32))
        return [jnp.broadcast_to(turned[:, i : i + 1], shape) for i in range(part.shape[0])]

    lon = lax.broadcasted_iota(jnp.int32, shape, 0)
    reverse = jnp.where(
        lax.broadcasted_iota(jnp.int32, (lons, lons), 0) + lax.broadcasted_iota(jnp.int32, (lons, lons), 1)
        == lons - 1,
        1.0,
        0.0,
    )

    def flip(part):
        return jnp.dot(
            reverse, part, preferred_element_type=jnp.float32, precision=lax.Precision.HIGHEST
        )

    is_top = gy == n_gy - 1
    wets = columns(mask[...])
    west_wets, east_wets = columns(masks[0]), columns(masks[1])
    south_wet = jnp.where(gy == 0, 0.0, columns(masks[2])[lats - 1])
    from_north = columns(masks[3])
    north_wet = jnp.where(is_top, flip(from_north[lats - 1]), from_north[0])
    south_state = jnp.where(gy == 0, 0.0, south[...].astype(jnp.float32))
    north_plain = north[...].astype(jnp.float32)
    north_state = jnp.where(is_top, flip(north_plain), north_plain)
    states = [state[i].astype(jnp.float32) for i in range(lats)]
    scale = mixing[...]
    for i in range(lats):
        center = states[i]
        from_west = jnp.broadcast_to(west[i].astype(jnp.float32)[-1:], shape)
        from_east = jnp.broadcast_to(east[i].astype(jnp.float32)[:1], shape)
        sides = (
            (
                jnp.where(lon == 0, from_west, pltpu.roll(center, 1, 0)),
                jnp.where(lon == 0, pltpu.roll(west_wets[i], 1, 0), pltpu.roll(wets[i], 1, 0)),
            ),
            (
                jnp.where(lon == lons - 1, from_east, pltpu.roll(center, lons - 1, 0)),
                jnp.where(
                    lon == lons - 1, pltpu.roll(east_wets[i], lons - 1, 0), pltpu.roll(wets[i], lons - 1, 0)
                ),
            ),
            (south_state, south_wet) if i == 0 else (states[i - 1], wets[i - 1]),
            (north_state, north_wet) if i == lats - 1 else (states[i + 1], wets[i + 1]),
        )
        diffusion = jnp.zeros_like(center)
        for side_state, side_wet in sides:
            diffusion = diffusion + side_wet * (side_state - center)
        wet[i] = wets[i]
        base[i] = wets[i] * (center + scale * diffusion)


def remap(count, positions, sources, firsts, targets, weight, blocks, state, mask, mixing, halo):
    smem = pl.BlockSpec(memory_space=pltpu.SMEM)
    vmem = pl.BlockSpec(memory_space=pltpu.VMEM)
    hbm = pl.BlockSpec(memory_space=pl.ANY)
    dma = pltpu.SemaphoreType.DMA
    return pl.pallas_call(
        remap_kernel,
        out_shape=jax.ShapeDtypeStruct(state.shape, state.dtype),
        in_specs=[smem, smem, smem, smem, smem, hbm, hbm] + [vmem] * 8,
        out_specs=vmem,
        scratch_shapes=[
            pltpu.VMEM((DEPTH, GROUP, ROWS, ROWS), jnp.bfloat16),
            pltpu.VMEM((DEPTH, GROUP, ROWS, CHANNELS), jnp.bfloat16),
            pltpu.VMEM((ROWS, 2 * CHANNELS), jnp.float32),
            pltpu.VMEM(state.shape, jnp.float32),
            pltpu.VMEM(state.shape, jnp.float32),
            dma((DEPTH,)),
            dma((DEPTH, GROUP)),
        ],
        compiler_params=pltpu.CompilerParams(vmem_limit_bytes=56 * 2**20),
        name="remap",
    )(count, positions, sources, firsts, targets, weight, blocks, state, mask, mixing, *halo)


def local(atm_fields, atm_pos, tile_src, tile_tgt, tile_count, tile_weight, ocean_state, land_mask, mixing):
    atm = atm_fields.reshape(BLOCKS, ROWS, CHANNELS)

    def finish(blocks, west, east, south, north, masks, firsts):
        return remap(
            tile_count, atm_pos, tile_src, firsts, tile_tgt, tile_weight, blocks.reshape(256, ROWS, CHANNELS),
            ocean_state, land_mask, mixing.reshape(1, CHANNELS), (west, east, south, north, masks),
        )

    *parts, over = lean_exchange(tile_count, atm_pos, tile_src, atm, ocean_state, land_mask)
    return lax.cond(
        over[0] > 0,
        lambda parts: finish(*exchange(atm_pos, tile_src, atm, ocean_state, land_mask)),
        lambda parts: finish(*parts),
        parts,
    )


def solution(mesh):
    both = ("gx", "gy")
    in_specs = (
        P(both, None),
        P(),
        P(both),
        P(both),
        P(both),
        P(both, None, None),
        P("gy", "gx", None),
        P("gy", "gx"),
        P(),
    )
    return jax.shard_map(
        local, mesh=mesh, in_specs=in_specs, out_specs=P("gy", "gx", None), check_vma=False
    )
```

```python
import functools

import jax
import jax.numpy as jnp
from jax import lax
from jax.experimental import pallas as pl
from jax.experimental.pallas import tpu as pltpu
from jax.sharding import PartitionSpec as P

MESH = pl.DeviceIdType.MESH
ROWS = 256
CHANNELS = 128
BLOCKS = 24
RING = 4
CORES = 2
CLASSES = ((0, 88, "xyz"), (88, 88, "yzx"), (176, 80, "zxy"))
FAR = (1, 3, 2)
GROUP = 8
LIST = 48
NOBODY = 31
DEPTH = 4
EXCHANGE_VMEM = 56 * 2**20


def peer(axis, offset, flip=0):
    gx, gy = lax.axis_index("gx"), lax.axis_index("gy")
    x, core, z, y = gx // 2, gx % 2, gy // 4, gy % 4
    if axis == "x":
        x = (x + offset) % RING
    if axis == "y":
        y = (y + offset) % RING
    if axis == "z":
        z = (z + offset) % RING
    core = (core + flip) % CORES
    return (x * 2 + core, z * 4 + y)


def where_from(position):
    gx, gy = lax.axis_index("gx"), lax.axis_index("gy")
    owner = lax.shift_right_logical(position * 2731, 16)
    ox, oy = lax.shift_right_logical(owner, 4), owner & 15
    dx = (gx // 2 - lax.shift_right_logical(ox, 1)) & 3
    dk = (gx - ox) & 1
    dz = (gy // 4 - lax.shift_right_logical(oy, 2)) & 3
    dy = (gy - oy) & 3
    return relative({"x": dx, "z": dz, "y": dy}, dk), position - owner * BLOCKS


def write_slots(slots, positions, sources, leaders):
    def body(tile, carry):
        lane, _ = where_from(positions[sources[tile]])
        slots[tile] = lane * 2 + jnp.where(leaders[0, lane] == tile, 0, 1)
        return carry

    lax.fori_loop(0, sources.shape[0], body, 0)


def relative(distance, core):
    return ((distance["x"] * CORES + core) * RING + distance["z"]) * RING + distance["y"]


def exchange_kernel(positions, sources, atm, state, mask, final, west, east, south, north, masks, slots, *scratch):
    kept, gathered, sent, relayed, first, second = (scratch[3 * i : 3 * i + 3] for i in range(6))
    (ask, table, ask_sem, ask_s, ask_r, mid_s, mid_r, smem_sem, own_sem, ag_s, ag_r,
     p2_s, p2_r, p3_s, p3_r, edge_s, edge_r, firsts, leaders, lead_sem) = scratch[18:]

    barrier = pltpu.get_barrier_semaphore()
    neighbours = [(a, o, f) for a in "xyz" for o in (1, 2, 3) for f in (0, 1)] + [("x", 0, 1)]
    for axis, offset, flip in neighbours:
        pl.semaphore_signal(barrier, 1, device_id=peer(axis, offset, flip), device_id_type=MESH)
    gx, gy = lax.axis_index("gx"), lax.axis_index("gy")
    n_gx, n_gy = lax.axis_size("gx"), lax.axis_size("gy")
    is_top = gy == n_gy - 1
    before, after = ((gx + n_gx - 1) % n_gx, gy), ((gx + 1) % n_gx, gy)
    above = (jnp.where(is_top, n_gx - 1 - gx, gx), jnp.where(is_top, gy, gy + 1))
    below = (gx, gy - 1)
    has_below = gy > 0
    for target in (before, after, above):
        pl.semaphore_signal(barrier, 1, device_id=target, device_id_type=MESH)

    @pl.when(has_below)
    def _():
        pl.semaphore_signal(barrier, 1, device_id=below, device_id_type=MESH)

    lane_of = lax.broadcasted_iota(jnp.int32, (1, 128), 1)
    zero = jnp.zeros((1, 128), jnp.int32)

    def claim(step, carry):
        count, ask0, ask1, leader = carry
        for i in range(8):
            tile = step * 8 + i
            lane, block = where_from(positions[sources[tile]])
            mine = lane_of == lane
            free = mine & (count == 0)
            ask0 = jnp.where(free, block, ask0)
            leader = jnp.where(free, tile, leader)
            ask1 = jnp.where(mine, jnp.where(free, ask1, block), ask1)
            count = jnp.where(mine, 1, count)
        return count, ask0, ask1, leader

    _, ask0, ask1, leader = lax.fori_loop(0, sources.shape[0] // 8, claim, (zero, zero, zero, zero))
    ask[0:1] = ask0
    ask[1:2] = ask1
    firsts[...] = leader

    pl.semaphore_wait(barrier, len(neighbours) + 3 + jnp.where(has_below, 1, 0))

    def copier(src, dst, send, recv, target):
        return pltpu.make_async_remote_copy(
            src_ref=src, dst_ref=dst, send_sem=send, recv_sem=recv, device_id=target, device_id_type=MESH
        )

    def remote(*parts):
        copy = copier(*parts)
        copy.start()
        return copy

    half = BLOCKS // 2
    low, high = pl.ds(0, half), pl.ds(half, half)

    def direct(c, i, offset, part):
        start, size, order = CLASSES[c]
        return remote(
            atm.at[part, pl.ds(start, size)], gathered[c].at[offset - 1, part],
            ag_s.at[c, i], ag_r.at[c, i], peer(order[0], offset),
        )

    def forward(c, i, origin, part):
        return remote(
            gathered[c].at[origin - 1, part], gathered[c].at[1, part],
            ag_s.at[c, i], ag_r.at[c, i], peer(CLASSES[c][2][0], origin),
        )

    rings = [[direct(c, 0, 1, low), direct(c, 1, 3, high)] for c in range(3)]
    owns = []
    for c, (start, size, _) in enumerate(CLASSES):
        own = pltpu.make_async_copy(atm.at[:, pl.ds(start, size)], kept[c], own_sem.at[c])
        own.start()
        owns.append(own)

    def edges(side, slot, target, src, dst):
        return (
            copier(src, dst, edge_s.at[0, side], edge_r.at[0, slot], target),
            copier(mask, masks.at[slot], edge_s.at[1, side], edge_r.at[1, slot], target),
        )

    last = state.shape[0] - 1
    wide = state.shape[1]
    to_before = edges(0, 1, before, state.at[:, pl.ds(0, 8)], east)
    to_after = edges(1, 0, after, state.at[:, pl.ds(wide - 8, 8)], west)
    to_below = edges(2, 3, below, state.at[0], north)
    to_fold = edges(3, 3, above, state.at[last], north)
    to_above = edges(3, 2, above, state.at[last], south)
    for copy in to_before + to_after:
        copy.start()
    for case, group in ((has_below, to_below), (is_top, to_fold), (jnp.logical_not(is_top), to_above)):

        @pl.when(case)
        def _():
            for copy in group:
                copy.start()

    asks, mids, p3s = [], [], []
    for c, (_, _, order) in enumerate(CLASSES):
        local = pltpu.make_async_copy(ask, first[c].at[0], ask_sem.at[c])
        local.start()
        asks.append([local])
        for lane in range(1, RING * CORES):
            o3, flip = lane // CORES, lane % CORES
            asks[c].append(
                remote(ask, first[c].at[lane], ask_s.at[c, lane], ask_r.at[c, lane], peer(order[2], -o3, flip))
            )
    for c in range(3):
        rings[c] += [direct(c, 2, 1, high), direct(c, 3, 3, low)]
    for c, (_, _, order) in enumerate(CLASSES):
        for copy in asks[c]:
            copy.wait()
        mids.append(
            [remote(first[c], second[c].at[o], mid_s.at[c, o], mid_r.at[c, o], peer(order[1], -o)) for o in FAR]
        )
        keep = pltpu.make_async_copy(first[c], table.at[c, 0], smem_sem.at[c, 0])
        keep.start()
        mids[c].append(keep)
    for c in range(3):
        for copy in rings[c][:2]:
            copy.wait()
        rings[c] = rings[c][2:] + [forward(c, 4, 1, low), forward(c, 5, 3, high)]
    keeps = []
    for c in range(3):
        for copy in mids[c]:
            copy.wait()
        for o in FAR:
            keep = pltpu.make_async_copy(second[c].at[o], table.at[c, o], smem_sem.at[c, o])
            keep.start()
            keeps.append(keep)
    for keep in keeps:
        keep.wait()

    def pack(c, o2, origins):
        order = CLASSES[c][2]

        def body(lane, carry):
            o3, flip = lane // CORES, lane % CORES
            for o1 in origins:
                for rank in range(2):
                    at = relative({order[0]: o1, order[1]: o2, order[2]: o3}, flip)
                    which = table[c, o2, lane, rank, at]
                    sent[c][o2, o1, lane, rank] = kept[c][which] if o1 == 0 else gathered[c][o1 - 1, which]
            return carry

        lax.fori_loop(0, RING * CORES, body, 0)

    def send2(c, o2, origins):
        order = CLASSES[c][2]
        part = pl.ds(origins[0], len(origins))
        i = 0 if origins[0] == 0 else 1
        return remote(
            sent[c].at[o2, part], relayed[c].at[o2, part], p2_s.at[c, o2, i], p2_r.at[c, o2, i],
            peer(order[1], o2),
        )

    def send3(c, o2):
        start, size, order = CLASSES[c]
        source = sent[c] if o2 == 0 else relayed[c]
        for lane in range(RING * CORES):
            o3, flip = lane // CORES, lane % CORES
            at = {order[0]: slice(None), order[1]: o2, order[2]: o3}
            dst = final.at[at["x"], flip, at["z"], at["y"], :, pl.ds(start, size)]
            src = source.at[o2, :, lane]
            if lane == 0:
                copy = pltpu.make_async_copy(src, dst, p3_s.at[c, o2, 0])
                copy.start()
                p3s.append(copy)
            else:
                p3s.append(
                    remote(src, dst, p3_s.at[c, o2, lane], p3_r.at[c, o2, lane], peer(order[2], o3, flip))
                )

    pending = {(c, o2): [] for c in range(3) for o2 in FAR}
    near, rest = (0,), (1, 2, 3)
    for owner in owns:
        owner.wait()
    last_step = None
    for origins in (near, rest):
        if origins is rest:
            for c in range(3):
                for copy in rings[c]:
                    copy.wait()
        for o2 in FAR:
            for c in range(3):
                pack(c, o2, origins)
                if last_step is not None:
                    pending[last_step[:2]].append(send2(*last_step))
                last_step = (c, o2, origins)
    for c in range(3):
        pack(c, 0, near + rest)
        if c == 0:
            pending[last_step[:2]].append(send2(*last_step))
        else:
            send3(c - 1, 0)
    lead = pltpu.make_async_copy(firsts, leaders, lead_sem)
    lead.start()
    lead.wait()
    write_slots(slots, positions, sources, leaders)
    for o2 in FAR:
        for c in range(3):
            for copy in pending[c, o2]:
                copy.wait()
            send3(c, o2)
            if (c, o2) == (0, 1):
                send3(2, 0)
    for copy in p3s:
        copy.wait()
    for copy in edges(0, 0, before, state.at[:, pl.ds(0, 8)], west) + edges(1, 1, after, state.at[:, pl.ds(0, 8)], east):
        copy.wait()
    for copy in edges(3, 3, above, state.at[last], north):
        copy.wait()

    @pl.when(has_below)
    def _():
        for copy in edges(2, 2, below, state.at[0], south):
            copy.wait()


def exchange(positions, sources, atm, state, mask):
    dma = pltpu.SemaphoreType.DMA
    tables = RING * CORES
    scratch = [pltpu.VMEM((BLOCKS, size, CHANNELS), jnp.bfloat16) for _, size, _ in CLASSES]
    scratch += [pltpu.VMEM((RING - 1, BLOCKS, size, CHANNELS), jnp.bfloat16) for _, size, _ in CLASSES]
    for _ in range(2):
        scratch += [
            pltpu.VMEM((RING, RING, tables, 2, size, CHANNELS), jnp.bfloat16) for _, size, _ in CLASSES
        ]
    scratch += [pltpu.VMEM((tables, 2, 128), jnp.int32) for _ in CLASSES]
    scratch += [pltpu.VMEM((RING, tables, 2, 128), jnp.int32) for _ in CLASSES]
    scratch += [
        pltpu.VMEM((2, 128), jnp.int32),
        pltpu.SMEM((3, RING, tables, 2, 128), jnp.int32),
        dma((3,)),
        dma((3, tables)),
        dma((3, tables)),
        dma((3, RING)),
        dma((3, RING)),
        dma((3, RING)),
        dma((3,)),
        dma((3, 6)),
        dma((3, 6)),
        dma((3, RING, 2)),
        dma((3, RING, 2)),
        dma((3, RING, tables)),
        dma((3, RING, tables)),
        dma((2, 4)),
        dma((2, 4)),
        pltpu.VMEM((1, 128), jnp.int32),
        pltpu.SMEM((1, 128), jnp.int32),
        dma,
    ]
    lat, lon = mask.shape
    smem = pl.BlockSpec(memory_space=pltpu.SMEM)
    vmem = pl.BlockSpec(memory_space=pltpu.VMEM)
    free = pl.BlockSpec(memory_space=pl.ANY)
    side = jax.ShapeDtypeStruct((lat, 8, CHANNELS), jnp.bfloat16)
    row = jax.ShapeDtypeStruct((lon, CHANNELS), jnp.bfloat16)
    return pl.pallas_call(
        exchange_kernel,
        out_shape=(
            jax.ShapeDtypeStruct((RING, CORES, RING, RING, 2, ROWS, CHANNELS), jnp.bfloat16),
            side,
            side,
            row,
            row,
            jax.ShapeDtypeStruct((4, lat, lon), jnp.int32),
            jax.ShapeDtypeStruct(sources.shape, jnp.int32),
        ),
        in_specs=[smem, smem, free, vmem, vmem],
        out_specs=(free, vmem, vmem, vmem, vmem, vmem, smem),
        scratch_shapes=scratch,
        compiler_params=pltpu.CompilerParams(
            collective_id=0, has_side_effects=True, vmem_limit_bytes=EXCHANGE_VMEM
        ),
        name="exchange",
    )(positions, sources, atm, state, mask)


def lean_kernel(
    count, positions, sources, atm, state, mask,
    final, west, east, south, north, masks, slots, flag, *scratch
):
    kept, gathered, sent, out3, first = (scratch[3 * i : 3 * i + 3] for i in range(5))
    relayed = [scratch[15 + 3 * c : 18 + 3 * c] for c in range(3)]
    (ask, needs, spots, lists, heard, over1, over2, over3, over1_in, over2_in, over3_in,
     table, spot_table, list_table, ask_sem, ask_s, ask_r, list_s, list_r, smem_sem, own_sem,
     ag_s, ag_r, p2_s, p2_r, p3_s, p3_r, edge_s, edge_r, over_s, over_r, firsts, leaders, lead_sem) = scratch[24:]

    barrier = pltpu.get_barrier_semaphore()
    neighbours = [(a, o, f) for a in "xyz" for o in (1, 2, 3) for f in (0, 1)] + [("x", 0, 1)]
    for axis, offset, flip in neighbours:
        pl.semaphore_signal(barrier, 1, device_id=peer(axis, offset, flip), device_id_type=MESH)
    gx, gy = lax.axis_index("gx"), lax.axis_index("gy")
    n_gx, n_gy = lax.axis_size("gx"), lax.axis_size("gy")
    is_top = gy == n_gy - 1
    before, after = ((gx + n_gx - 1) % n_gx, gy), ((gx + 1) % n_gx, gy)
    above = (jnp.where(is_top, n_gx - 1 - gx, gx), jnp.where(is_top, gy, gy + 1))
    below = (gx, gy - 1)
    has_below = gy > 0
    for target in (before, after, above):
        pl.semaphore_signal(barrier, 1, device_id=target, device_id_type=MESH)

    @pl.when(has_below)
    def _():
        pl.semaphore_signal(barrier, 1, device_id=below, device_id_type=MESH)

    lane_of = lax.broadcasted_iota(jnp.int32, (1, 128), 1)
    zero = jnp.zeros((1, 128), jnp.int32)
    live = count[0]

    def claim(step, carry):
        taken, ask0, ask1, leader = carry
        for i in range(8):
            tile = step * 8 + i
            lane, block = where_from(positions[sources[tile]])
            mine = lane_of == jnp.where(tile < live, lane, 128)
            free = mine & (taken == 0)
            ask0 = jnp.where(free, block, ask0)
            leader = jnp.where(free, tile, leader)
            ask1 = jnp.where(mine, jnp.where(free, ask1, block), ask1)
            taken = jnp.where(mine, 1, taken)
        return taken, ask0, ask1, leader

    _, ask0, ask1, leader = lax.fori_loop(
        0, sources.shape[0] // 8, claim, (zero, zero + NOBODY, zero + NOBODY, zero)
    )
    ask[0:1] = ask0
    ask[1:2] = ask1
    firsts[...] = leader
    pl.semaphore_wait(barrier, len(neighbours) + 3 + jnp.where(has_below, 1, 0))

    def copier(src, dst, send, recv, target):
        return pltpu.make_async_remote_copy(
            src_ref=src, dst_ref=dst, send_sem=send, recv_sem=recv, device_id=target, device_id_type=MESH
        )

    def remote(*parts):
        copy = copier(*parts)
        copy.start()
        return copy

    def keep(src, dst, sem):
        copy = pltpu.make_async_copy(src, dst, sem)
        copy.start()
        return copy

    half = BLOCKS // 2
    low, high = pl.ds(0, half), pl.ds(half, half)

    def direct(c, i, offset, part):
        start, size, order = CLASSES[c]
        return remote(
            atm.at[part, pl.ds(start, size)], gathered[c].at[offset, part],
            ag_s.at[c, i], ag_r.at[c, i], peer(order[0], offset),
        )

    def forward(c, i, origin, part):
        return remote(
            gathered[c].at[origin, part], gathered[c].at[2, part],
            ag_s.at[c, i], ag_r.at[c, i], peer(CLASSES[c][2][0], origin),
        )

    rings = [[direct(c, 0, 1, low), direct(c, 1, 3, high)] for c in range(3)]
    owns = []
    for c, (start, size, _) in enumerate(CLASSES):
        owns.append(keep(atm.at[:, pl.ds(start, size)], kept[c], own_sem.at[c, 0]))
        rings[c].append(keep(atm.at[:, pl.ds(start, size)], gathered[c].at[0], own_sem.at[c, 1]))

    def edges(side, slot, target, src, dst):
        return (
            copier(src, dst, edge_s.at[0, side], edge_r.at[0, slot], target),
            copier(mask, masks.at[slot], edge_s.at[1, side], edge_r.at[1, slot], target),
        )

    last = state.shape[0] - 1
    wide = state.shape[1]
    to_before = edges(0, 1, before, state.at[:, pl.ds(0, 8)], east)
    to_after = edges(1, 0, after, state.at[:, pl.ds(wide - 8, 8)], west)
    to_below = edges(2, 3, below, state.at[0], north)
    to_fold = edges(3, 3, above, state.at[last], north)
    to_above = edges(3, 2, above, state.at[last], south)
    for copy in to_before + to_after:
        copy.start()
    for case, group in ((has_below, to_below), (is_top, to_fold), (jnp.logical_not(is_top), to_above)):

        @pl.when(case)
        def _():
            for copy in group:
                copy.start()

    asks = []
    for c, (_, _, order) in enumerate(CLASSES):
        asks.append([keep(ask, first[c].at[0], ask_sem.at[c])])
        for lane in range(1, RING * CORES):
            o3, flip = lane // CORES, lane % CORES
            asks[c].append(
                remote(ask, first[c].at[lane], ask_s.at[c, lane], ask_r.at[c, lane], peer(order[2], -o3, flip))
            )
    for c in range(3):
        rings[c] += [direct(c, 2, 1, high), direct(c, 3, 3, low)]

    def wanted(c, o1, o2, lane, rank):
        order = CLASSES[c][2]
        o3, flip = lane // CORES, lane % CORES
        return table[c, lane, rank, relative({order[0]: o1, order[1]: o2, order[2]: o3}, flip)]

    keeps = []
    for c in range(3):
        for copy in asks[c]:
            copy.wait()
        keeps.append(keep(first[c], table.at[c], smem_sem.at[0, c]))
    needs[...] = jnp.zeros_like(needs)
    for c in range(3):
        keeps[c].wait()

        def mark(lane, seen):
            seen = list(seen)
            for o2 in FAR:
                for o1 in range(RING):
                    for rank in range(2):
                        key = o1 * 32 + wanted(c, o1, o2, lane, rank)
                        seen[o2 - 1] = jnp.where(lane_of == key, 1, seen[o2 - 1])
            return tuple(seen)

        seen = lax.fori_loop(0, RING * CORES, mark, (zero, zero, zero))
        for o2 in FAR:
            row = c * 3 + o2 - 1
            needs[row : row + 1] = jnp.where((lane_of & 31) < BLOCKS, seen[o2 - 1], 0)

    need = needs[...]
    upper = lax.broadcasted_iota(jnp.int32, (128, 128), 0) < lax.broadcasted_iota(jnp.int32, (128, 128), 1)
    spot = jnp.dot(
        need.astype(jnp.float32).astype(jnp.bfloat16),
        jnp.where(upper, 1.0, 0.0).astype(jnp.bfloat16),
        preferred_element_type=jnp.float32,
    ).astype(jnp.int32)
    over1[...] = jnp.where((need > 0) & (spot >= LIST), 1, 0)
    spots[...] = jnp.clip(spot, 0, LIST - 1)
    keys = lax.broadcasted_iota(jnp.int32, (8, 128), 1).astype(jnp.float32).astype(jnp.bfloat16)
    place = lax.broadcasted_iota(jnp.int32, (128, 128), 0)
    for row in range(9):
        mine = (spot[row : row + 1] == place) & (need[row : row + 1] > 0)
        lists[row] = lax.dot_general(
            keys,
            jnp.where(mine, 1.0, 0.0).astype(jnp.bfloat16),
            (((1,), (1,)), ((), ())),
            preferred_element_type=jnp.float32,
        ).astype(jnp.int32)

    def pack3(c, o2, origins):
        def body(lane, carry):
            for o1 in origins:
                for rank in range(2):
                    which = wanted(c, o1, o2, lane, rank) & 31
                    if o2:
                        at = jnp.clip(spot_table[c * 3 + o2 - 1, o1 * 32 + which], 0, LIST - 1)
                        block = relayed[c][o2 - 1][at]
                    elif o1 == 0:
                        block = kept[c][jnp.minimum(which, BLOCKS - 1)]
                    else:
                        block = gathered[c][o1, jnp.minimum(which, BLOCKS - 1)]
                    out3[c][o2, lane, o1, rank] = block
            return carry

        lax.fori_loop(0, RING * CORES, body, 0)

    p3s = []

    def send3(c, o2, origins, part):
        start, size, order = CLASSES[c]
        span = pl.ds(origins[0], len(origins))
        for lane in range(RING * CORES):
            o3, flip = lane // CORES, lane % CORES
            at = {order[0]: span, order[1]: o2, order[2]: o3}
            dst = final.at[at["x"], flip, at["z"], at["y"], :, pl.ds(start, size)]
            src = out3[c].at[o2, lane, span]
            if lane == 0:
                p3s.append(keep(src, dst, p3_s.at[c, part, 0]))
            else:
                p3s.append(
                    remote(src, dst, p3_s.at[c, part, lane], p3_r.at[c, part, lane], peer(order[2], o3, flip))
                )

    near, rest, every = (0,), (1, 2, 3), (0, 1, 2, 3)
    spot_keep = keep(spots, spot_table, smem_sem.at[1, 0])
    for owner in owns:
        owner.wait()
    pack3(0, 0, near)
    tells = []
    for c, (_, _, order) in enumerate(CLASSES):
        for o2 in FAR:
            row = c * 3 + o2 - 1
            tells.append(
                remote(lists.at[row], heard.at[row], list_s.at[row], list_r.at[row], peer(order[1], -o2))
            )
    circle = [(o, f) for o in range(RING) for f in range(CORES) if o or f]
    votes = [
        remote(over1, over1_in.at[i], over_s.at[i], over_r.at[i], peer("x", o, f))
        for i, (o, f) in enumerate(circle)
    ]
    for c in range(3):
        for copy in rings[c][:3]:
            copy.wait()
        rings[c] = rings[c][3:] + [forward(c, 4, 1, low), forward(c, 5, 3, high)]
    pack3(1, 0, near)
    send3(0, 0, near, 4)
    pack3(2, 0, near)
    send3(1, 0, near, 4)
    for row, copy in enumerate(tells):
        copy.wait()
    list_keep = keep(heard, list_table, smem_sem.at[1, 1])
    send3(2, 0, near, 4)
    list_keep.wait()
    spot_keep.wait()
    for c in range(3):
        for copy in rings[c]:
            copy.wait()

    def pack2(c, o2):
        row = c * 3 + o2 - 1

        def body(step, carry):
            for i in range(8):
                slot = step * 8 + i
                key = list_table[row, 0, slot]
                origin = lax.shift_right_logical(key, 5)
                sent[c][o2 - 1, slot] = gathered[c][origin & 3, jnp.minimum(key & 31, BLOCKS - 1)]
            return carry

        lax.fori_loop(0, LIST // 8, body, 0)

    def send2(c, o2):
        return remote(
            sent[c].at[o2 - 1], relayed[c][o2 - 1], p2_s.at[c, o2 - 1], p2_r.at[c, o2 - 1],
            peer(CLASSES[c][2][1], o2),
        )

    steps = [(c, o2) for o2 in FAR for c in range(3)]
    pending = {}
    for i, step in enumerate(steps):
        pack2(*step)
        if i:
            pending[steps[i - 1]] = send2(*steps[i - 1])
    pack3(0, 0, rest)
    pending[steps[-1]] = send2(*steps[-1])
    for copy in votes:
        copy.wait()
    over2[...] = functools.reduce(jnp.maximum, [over1_in[i] for i in range(len(circle))], over1[...])
    pack3(1, 0, rest)
    send3(0, 0, rest, 0)
    pack3(2, 0, rest)
    send3(1, 0, rest, 0)
    votes = [
        remote(over2, over2_in.at[o - 1], over_s.at[7 + o - 1], over_r.at[7 + o - 1], peer("y", o)) for o in FAR
    ]
    send3(2, 0, rest, 0)
    keep(firsts, leaders, lead_sem).wait()
    write_slots(slots, positions, sources, leaders)
    for i, (c, o2) in enumerate(steps):
        pending[c, o2].wait()
        pack3(c, o2, every)
        send3(c, o2, every, o2)
        if i == 2:
            for copy in votes:
                copy.wait()
            over3[...] = functools.reduce(jnp.maximum, [over2_in[k] for k in range(3)], over2[...])
        if i == 3:
            votes = [
                remote(over3, over3_in.at[o - 1], over_s.at[10 + o - 1], over_r.at[10 + o - 1], peer("z", o))
                for o in FAR
            ]
    for copy in votes:
        copy.wait()
    verdict = functools.reduce(jnp.maximum, [over3_in[k] for k in range(3)], over3[...])
    flag[0] = jnp.max(verdict)
    for copy in p3s:
        copy.wait()
    for copy in edges(0, 0, before, state.at[:, pl.ds(0, 8)], west) + edges(1, 1, after, state.at[:, pl.ds(0, 8)], east):
        copy.wait()
    for copy in edges(3, 3, above, state.at[last], north):
        copy.wait()

    @pl.when(has_below)
    def _():
        for copy in edges(2, 2, below, state.at[0], south):
            copy.wait()


def lean_exchange(count, positions, sources, atm, state, mask):
    dma = pltpu.SemaphoreType.DMA
    tables = RING * CORES
    sizes = [size for _, size, _ in CLASSES]
    scratch = [pltpu.VMEM((BLOCKS, size, CHANNELS), jnp.bfloat16) for size in sizes]
    scratch += [pltpu.VMEM((RING, BLOCKS, size, CHANNELS), jnp.bfloat16) for size in sizes]
    scratch += [pltpu.VMEM((3, LIST, size, CHANNELS), jnp.bfloat16) for size in sizes]
    scratch += [pltpu.VMEM((RING, tables, RING, 2, size, CHANNELS), jnp.bfloat16) for size in sizes]
    scratch += [pltpu.VMEM((tables, 2, 128), jnp.int32) for _ in sizes]
    for size in sizes:
        scratch += [pltpu.VMEM((LIST, size, CHANNELS), jnp.bfloat16) for _ in range(3)]
    votes = pltpu.VMEM((16, 128), jnp.int32)
    scratch += [
        pltpu.VMEM((2, 128), jnp.int32),
        votes,
        votes,
        pltpu.VMEM((9, 8, 128), jnp.int32),
        pltpu.VMEM((9, 8, 128), jnp.int32),
        votes,
        votes,
        votes,
        pltpu.VMEM((7, 16, 128), jnp.int32),
        pltpu.VMEM((3, 16, 128), jnp.int32),
        pltpu.VMEM((3, 16, 128), jnp.int32),
        pltpu.SMEM((3, tables, 2, 128), jnp.int32),
        pltpu.SMEM((16, 128), jnp.int32),
        pltpu.SMEM((9, 8, 128), jnp.int32),
        dma((3,)),
        dma((3, tables)),
        dma((3, tables)),
        dma((9,)),
        dma((9,)),
        dma((2, 3)),
        dma((3, 2)),
        dma((3, 6)),
        dma((3, 6)),
        dma((3, 3)),
        dma((3, 3)),
        dma((3, RING + 1, tables)),
        dma((3, RING + 1, tables)),
        dma((2, 4)),
        dma((2, 4)),
        dma((13,)),
        dma((13,)),
        pltpu.VMEM((1, 128), jnp.int32),
        pltpu.SMEM((1, 128), jnp.int32),
        dma,
    ]
    lat, lon = mask.shape
    smem = pl.BlockSpec(memory_space=pltpu.SMEM)
    vmem = pl.BlockSpec(memory_space=pltpu.VMEM)
    free = pl.BlockSpec(memory_space=pl.ANY)
    hbm = pl.BlockSpec(memory_space=pltpu.HBM)
    side = jax.ShapeDtypeStruct((lat, 8, CHANNELS), jnp.bfloat16)
    row = jax.ShapeDtypeStruct((lon, CHANNELS), jnp.bfloat16)
    return pl.pallas_call(
        lean_kernel,
        out_shape=(
            jax.ShapeDtypeStruct((RING, CORES, RING, RING, 2, ROWS, CHANNELS), jnp.bfloat16),
            side,
            side,
            row,
            row,
            jax.ShapeDtypeStruct((4, lat, lon), jnp.int32),
            jax.ShapeDtypeStruct(sources.shape, jnp.int32),
            jax.ShapeDtypeStruct((1,), jnp.int32),
        ),
        in_specs=[smem, smem, smem, free, hbm, hbm],
        out_specs=(free, hbm, hbm, hbm, hbm, hbm, smem, smem),
        scratch_shapes=scratch,
        compiler_params=pltpu.CompilerParams(
            collective_id=1, has_side_effects=True, vmem_limit_bytes=EXCHANGE_VMEM
        ),
        name="lean_exchange",
    )(count, positions, sources, atm, state, mask)


def remap_kernel(
    count, slots, targets, weight, blocks, state, mask, mixing,
    west, east, south, north, masks, out, w_buf, x_buf, total, base, wet, w_sem, x_sem,
):
    live = count[0]
    steps = (live + GROUP - 1) // GROUP

    def copies(step, at, started=False):
        first = step * GROUP
        yield pltpu.make_async_copy(weight.at[pl.ds(first, GROUP)], w_buf.at[at], w_sem.at[at])
        for i in range(GROUP):
            slot = slots[first + i] if started else 0
            yield pltpu.make_async_copy(blocks.at[slot], x_buf.at[at, i], x_sem.at[at, i])

    def fetch(step):
        @pl.when(step < steps)
        def _():
            for copy in copies(step, lax.rem(step, DEPTH), True):
                copy.start()

    for step in range(DEPTH - 1):
        fetch(step)
    total[...] = jnp.zeros_like(total)
    stencil(state, mask, mixing, west, east, south, north, masks, base, wet)

    def body(step, carry):
        at = lax.rem(step, DEPTH)
        fetch(step + DEPTH - 1)
        for copy in copies(step, at):
            copy.wait()
        zero = jnp.zeros((ROWS, CHANNELS), jnp.bfloat16)
        right = []
        for i in range(GROUP):
            tile = step * GROUP + i
            target = jnp.where(tile < live, targets[tile], 2)
            x = x_buf[at, i]
            right.append(
                jnp.concatenate([jnp.where(target == b, x, zero) for b in range(2)], axis=1)
            )
        left = jnp.concatenate([w_buf[at, i] for i in range(GROUP)], axis=1)
        total[...] += jnp.dot(
            left, jnp.concatenate(right, axis=0), preferred_element_type=jnp.float32
        )
        return carry

    lax.fori_loop(0, steps, body, 0)
    lats, lons, _ = state.shape
    for i in range(lats):
        row = i * lons % ROWS
        b = i * lons // ROWS
        forcing = total[row : row + lons, b * CHANNELS : (b + 1) * CHANNELS]
        out[i] = (base[i] + wet[i] * forcing).astype(out.dtype)


def stencil(state, mask, mixing, west, east, south, north, masks, base, wet):
    gy, n_gy = lax.axis_index("gy"), lax.axis_size("gy")
    lats, lons, channels = state.shape
    shape = (lons, channels)

    def columns(part):
        turned = jnp.transpose(part.astype(jnp.float32))
        return [jnp.broadcast_to(turned[:, i : i + 1], shape) for i in range(part.shape[0])]

    lon = lax.broadcasted_iota(jnp.int32, shape, 0)
    reverse = jnp.where(
        lax.broadcasted_iota(jnp.int32, (lons, lons), 0) + lax.broadcasted_iota(jnp.int32, (lons, lons), 1)
        == lons - 1,
        1.0,
        0.0,
    )

    def flip(part):
        return jnp.dot(
            reverse, part, preferred_element_type=jnp.float32, precision=lax.Precision.HIGHEST
        )

    is_top = gy == n_gy - 1
    wets = columns(mask[...])
    west_wets, east_wets = columns(masks[0]), columns(masks[1])
    south_wet = jnp.where(gy == 0, 0.0, columns(masks[2])[lats - 1])
    from_north = columns(masks[3])
    north_wet = jnp.where(is_top, flip(from_north[lats - 1]), from_north[0])
    south_state = jnp.where(gy == 0, 0.0, south[...].astype(jnp.float32))
    north_plain = north[...].astype(jnp.float32)
    north_state = jnp.where(is_top, flip(north_plain), north_plain)
    states = [state[i].astype(jnp.float32) for i in range(lats)]
    scale = mixing[...]
    for i in range(lats):
        center = states[i]
        from_west = jnp.broadcast_to(west[i].astype(jnp.float32)[-1:], shape)
        from_east = jnp.broadcast_to(east[i].astype(jnp.float32)[:1], shape)
        sides = (
            (
                jnp.where(lon == 0, from_west, pltpu.roll(center, 1, 0)),
                jnp.where(lon == 0, pltpu.roll(west_wets[i], 1, 0), pltpu.roll(wets[i], 1, 0)),
            ),
            (
                jnp.where(lon == lons - 1, from_east, pltpu.roll(center, lons - 1, 0)),
                jnp.where(
                    lon == lons - 1, pltpu.roll(east_wets[i], lons - 1, 0), pltpu.roll(wets[i], lons - 1, 0)
                ),
            ),
            (south_state, south_wet) if i == 0 else (states[i - 1], wets[i - 1]),
            (north_state, north_wet) if i == lats - 1 else (states[i + 1], wets[i + 1]),
        )
        diffusion = jnp.zeros_like(center)
        for side_state, side_wet in sides:
            diffusion = diffusion + side_wet * (side_state - center)
        wet[i] = wets[i]
        base[i] = wets[i] * (center + scale * diffusion)


def remap(count, slots, targets, weight, blocks, state, mask, mixing, halo):
    smem = pl.BlockSpec(memory_space=pltpu.SMEM)
    vmem = pl.BlockSpec(memory_space=pltpu.VMEM)
    hbm = pl.BlockSpec(memory_space=pl.ANY)
    dma = pltpu.SemaphoreType.DMA
    return pl.pallas_call(
        remap_kernel,
        out_shape=jax.ShapeDtypeStruct(state.shape, state.dtype),
        in_specs=[smem, smem, smem, hbm, hbm] + [vmem] * 8,
        out_specs=vmem,
        scratch_shapes=[
            pltpu.VMEM((DEPTH, GROUP, ROWS, ROWS), jnp.bfloat16),
            pltpu.VMEM((DEPTH, GROUP, ROWS, CHANNELS), jnp.bfloat16),
            pltpu.VMEM((ROWS, 2 * CHANNELS), jnp.float32),
            pltpu.VMEM(state.shape, jnp.float32),
            pltpu.VMEM(state.shape, jnp.float32),
            dma((DEPTH,)),
            dma((DEPTH, GROUP)),
        ],
        compiler_params=pltpu.CompilerParams(vmem_limit_bytes=56 * 2**20),
        name="remap",
    )(count, slots, targets, weight, blocks, state, mask, mixing, *halo)


def local(atm_fields, atm_pos, tile_src, tile_tgt, tile_count, tile_weight, ocean_state, land_mask, mixing):
    atm = atm_fields.reshape(BLOCKS, ROWS, CHANNELS)

    def finish(blocks, west, east, south, north, masks, slots):
        return remap(
            tile_count, slots, tile_tgt, tile_weight, blocks.reshape(256, ROWS, CHANNELS),
            ocean_state, land_mask, mixing.reshape(1, CHANNELS), (west, east, south, north, masks),
        )

    *parts, over = lean_exchange(tile_count, atm_pos, tile_src, atm, ocean_state, land_mask)
    return lax.cond(
        over.reshape(()) > 0,
        lambda parts: finish(*exchange(atm_pos, tile_src, atm, ocean_state, land_mask)),
        lambda parts: finish(*parts),
        parts,
    )


def solution(mesh):
    both = ("gx", "gy")
    in_specs = (
        P(both, None),
        P(),
        P(both),
        P(both),
        P(both),
        P(both, None, None),
        P("gy", "gx", None),
        P("gy", "gx"),
        P(),
    )
    return jax.shard_map(
        local, mesh=mesh, in_specs=in_specs, out_specs=P("gy", "gx", None), check_vma=False
    )
```

```python
import functools

import jax
import jax.numpy as jnp
from jax import lax
from jax.experimental import pallas as pl
from jax.experimental.pallas import tpu as pltpu
from jax.sharding import PartitionSpec as P

MESH = pl.DeviceIdType.MESH
ROWS = 256
CHANNELS = 128
BLOCKS = 24
RING = 4
CORES = 2
CLASSES = ((0, 88, "xyz"), (88, 88, "yzx"), (176, 80, "zxy"))
FAR = (2, 1, 3)
GROUP = 8
LIST = 48
NOBODY = 31
DEPTH = 4
EXCHANGE_VMEM = 56 * 2**20


def peer(axis, offset, flip=0):
    gx, gy = lax.axis_index("gx"), lax.axis_index("gy")
    x, core, z, y = gx // 2, gx % 2, gy // 4, gy % 4
    if axis == "x":
        x = (x + offset) % RING
    if axis == "y":
        y = (y + offset) % RING
    if axis == "z":
        z = (z + offset) % RING
    core = (core + flip) % CORES
    return (x * 2 + core, z * 4 + y)


def where_from(position):
    gx, gy = lax.axis_index("gx"), lax.axis_index("gy")
    owner = lax.shift_right_logical(position * 2731, 16)
    ox, oy = lax.shift_right_logical(owner, 4), owner & 15
    dx = (gx // 2 - lax.shift_right_logical(ox, 1)) & 3
    dk = (gx - ox) & 1
    dz = (gy // 4 - lax.shift_right_logical(oy, 2)) & 3
    dy = (gy - oy) & 3
    return relative({"x": dx, "z": dz, "y": dy}, dk), position - owner * BLOCKS


def write_slots(slots, positions, sources, leaders):
    def body(tile, carry):
        lane, _ = where_from(positions[sources[tile]])
        slots[tile] = lane * 2 + jnp.where(leaders[0, lane] == tile, 0, 1)
        return carry

    lax.fori_loop(0, sources.shape[0], body, 0)


def relative(distance, core):
    return ((distance["x"] * CORES + core) * RING + distance["z"]) * RING + distance["y"]


def exchange_kernel(positions, sources, atm, state, mask, final, west, east, south, north, masks, slots, *scratch):
    kept, gathered, sent, relayed, first, second = (scratch[3 * i : 3 * i + 3] for i in range(6))
    (ask, table, ask_sem, ask_s, ask_r, mid_s, mid_r, smem_sem, own_sem, ag_s, ag_r,
     p2_s, p2_r, p3_s, p3_r, edge_s, edge_r, firsts, leaders, lead_sem) = scratch[18:]

    barrier = pltpu.get_barrier_semaphore()
    neighbours = [(a, o, f) for a in "xyz" for o in (1, 2, 3) for f in (0, 1)] + [("x", 0, 1)]
    for axis, offset, flip in neighbours:
        pl.semaphore_signal(barrier, 1, device_id=peer(axis, offset, flip), device_id_type=MESH)
    gx, gy = lax.axis_index("gx"), lax.axis_index("gy")
    n_gx, n_gy = lax.axis_size("gx"), lax.axis_size("gy")
    is_top = gy == n_gy - 1
    before, after = ((gx + n_gx - 1) % n_gx, gy), ((gx + 1) % n_gx, gy)
    above = (jnp.where(is_top, n_gx - 1 - gx, gx), jnp.where(is_top, gy, gy + 1))
    below = (gx, gy - 1)
    has_below = gy > 0
    for target in (before, after, above):
        pl.semaphore_signal(barrier, 1, device_id=target, device_id_type=MESH)

    @pl.when(has_below)
    def _():
        pl.semaphore_signal(barrier, 1, device_id=below, device_id_type=MESH)

    lane_of = lax.broadcasted_iota(jnp.int32, (1, 128), 1)
    zero = jnp.zeros((1, 128), jnp.int32)

    def claim(step, carry):
        count, ask0, ask1, leader = carry
        for i in range(8):
            tile = step * 8 + i
            lane, block = where_from(positions[sources[tile]])
            mine = lane_of == lane
            free = mine & (count == 0)
            ask0 = jnp.where(free, block, ask0)
            leader = jnp.where(free, tile, leader)
            ask1 = jnp.where(mine, jnp.where(free, ask1, block), ask1)
            count = jnp.where(mine, 1, count)
        return count, ask0, ask1, leader

    _, ask0, ask1, leader = lax.fori_loop(0, sources.shape[0] // 8, claim, (zero, zero, zero, zero))
    ask[0:1] = ask0
    ask[1:2] = ask1
    firsts[...] = leader

    pl.semaphore_wait(barrier, len(neighbours) + 3 + jnp.where(has_below, 1, 0))

    def copier(src, dst, send, recv, target):
        return pltpu.make_async_remote_copy(
            src_ref=src, dst_ref=dst, send_sem=send, recv_sem=recv, device_id=target, device_id_type=MESH
        )

    def remote(*parts):
        copy = copier(*parts)
        copy.start()
        return copy

    half = BLOCKS // 2
    low, high = pl.ds(0, half), pl.ds(half, half)

    def direct(c, i, offset, part):
        start, size, order = CLASSES[c]
        return remote(
            atm.at[part, pl.ds(start, size)], gathered[c].at[offset - 1, part],
            ag_s.at[c, i], ag_r.at[c, i], peer(order[0], offset),
        )

    def forward(c, i, origin, part):
        return remote(
            gathered[c].at[origin - 1, part], gathered[c].at[1, part],
            ag_s.at[c, i], ag_r.at[c, i], peer(CLASSES[c][2][0], origin),
        )

    rings = [[direct(c, 0, 1, low), direct(c, 1, 3, high)] for c in range(3)]
    owns = []
    for c, (start, size, _) in enumerate(CLASSES):
        own = pltpu.make_async_copy(atm.at[:, pl.ds(start, size)], kept[c], own_sem.at[c])
        own.start()
        owns.append(own)

    def edges(side, slot, target, src, dst):
        return (
            copier(src, dst, edge_s.at[0, side], edge_r.at[0, slot], target),
            copier(mask, masks.at[slot], edge_s.at[1, side], edge_r.at[1, slot], target),
        )

    last = state.shape[0] - 1
    wide = state.shape[1]
    to_before = edges(0, 1, before, state.at[:, pl.ds(0, 8)], east)
    to_after = edges(1, 0, after, state.at[:, pl.ds(wide - 8, 8)], west)
    to_below = edges(2, 3, below, state.at[0], north)
    to_fold = edges(3, 3, above, state.at[last], north)
    to_above = edges(3, 2, above, state.at[last], south)
    for copy in to_before + to_after:
        copy.start()
    for case, group in ((has_below, to_below), (is_top, to_fold), (jnp.logical_not(is_top), to_above)):

        @pl.when(case)
        def _():
            for copy in group:
                copy.start()

    asks, mids, p3s = [], [], []
    for c, (_, _, order) in enumerate(CLASSES):
        local = pltpu.make_async_copy(ask, first[c].at[0], ask_sem.at[c])
        local.start()
        asks.append([local])
        for lane in range(1, RING * CORES):
            o3, flip = lane // CORES, lane % CORES
            asks[c].append(
                remote(ask, first[c].at[lane], ask_s.at[c, lane], ask_r.at[c, lane], peer(order[2], -o3, flip))
            )
    for c in range(3):
        rings[c] += [direct(c, 2, 1, high), direct(c, 3, 3, low)]
    for c, (_, _, order) in enumerate(CLASSES):
        for copy in asks[c]:
            copy.wait()
        mids.append(
            [remote(first[c], second[c].at[o], mid_s.at[c, o], mid_r.at[c, o], peer(order[1], -o)) for o in FAR]
        )
        keep = pltpu.make_async_copy(first[c], table.at[c, 0], smem_sem.at[c, 0])
        keep.start()
        mids[c].append(keep)
    for c in range(3):
        for copy in rings[c][:2]:
            copy.wait()
        rings[c] = rings[c][2:] + [forward(c, 4, 1, low), forward(c, 5, 3, high)]
    keeps = []
    for c in range(3):
        for copy in mids[c]:
            copy.wait()
        for o in FAR:
            keep = pltpu.make_async_copy(second[c].at[o], table.at[c, o], smem_sem.at[c, o])
            keep.start()
            keeps.append(keep)
    for keep in keeps:
        keep.wait()

    def pack(c, o2, origins):
        order = CLASSES[c][2]

        def body(lane, carry):
            o3, flip = lane // CORES, lane % CORES
            for o1 in origins:
                for rank in range(2):
                    at = relative({order[0]: o1, order[1]: o2, order[2]: o3}, flip)
                    which = table[c, o2, lane, rank, at]
                    sent[c][o2, o1, lane, rank] = kept[c][which] if o1 == 0 else gathered[c][o1 - 1, which]
            return carry

        lax.fori_loop(0, RING * CORES, body, 0)

    def send2(c, o2, origins):
        order = CLASSES[c][2]
        part = pl.ds(origins[0], len(origins))
        i = 0 if origins[0] == 0 else 1
        return remote(
            sent[c].at[o2, part], relayed[c].at[o2, part], p2_s.at[c, o2, i], p2_r.at[c, o2, i],
            peer(order[1], o2),
        )

    def send3(c, o2):
        start, size, order = CLASSES[c]
        source = sent[c] if o2 == 0 else relayed[c]
        for lane in range(RING * CORES):
            o3, flip = lane // CORES, lane % CORES
            at = {order[0]: slice(None), order[1]: o2, order[2]: o3}
            dst = final.at[at["x"], flip, at["z"], at["y"], :, pl.ds(start, size)]
            src = source.at[o2, :, lane]
            if lane == 0:
                copy = pltpu.make_async_copy(src, dst, p3_s.at[c, o2, 0])
                copy.start()
                p3s.append(copy)
            else:
                p3s.append(
                    remote(src, dst, p3_s.at[c, o2, lane], p3_r.at[c, o2, lane], peer(order[2], o3, flip))
                )

    pending = {(c, o2): [] for c in range(3) for o2 in FAR}
    near, rest = (0,), (1, 2, 3)
    for owner in owns:
        owner.wait()
    last_step = None
    for origins in (near, rest):
        if origins is rest:
            for c in range(3):
                for copy in rings[c]:
                    copy.wait()
        for o2 in FAR:
            for c in range(3):
                pack(c, o2, origins)
                if last_step is not None:
                    pending[last_step[:2]].append(send2(*last_step))
                last_step = (c, o2, origins)
    for c in range(3):
        pack(c, 0, near + rest)
        if c == 0:
            pending[last_step[:2]].append(send2(*last_step))
        else:
            send3(c - 1, 0)
    lead = pltpu.make_async_copy(firsts, leaders, lead_sem)
    lead.start()
    lead.wait()
    write_slots(slots, positions, sources, leaders)
    for o2 in FAR:
        for c in range(3):
            for copy in pending[c, o2]:
                copy.wait()
            send3(c, o2)
            if (c, o2) == (0, 1):
                send3(2, 0)
    for copy in p3s:
        copy.wait()
    for copy in edges(0, 0, before, state.at[:, pl.ds(0, 8)], west) + edges(1, 1, after, state.at[:, pl.ds(0, 8)], east):
        copy.wait()
    for copy in edges(3, 3, above, state.at[last], north):
        copy.wait()

    @pl.when(has_below)
    def _():
        for copy in edges(2, 2, below, state.at[0], south):
            copy.wait()


def exchange(positions, sources, atm, state, mask):
    dma = pltpu.SemaphoreType.DMA
    tables = RING * CORES
    scratch = [pltpu.VMEM((BLOCKS, size, CHANNELS), jnp.bfloat16) for _, size, _ in CLASSES]
    scratch += [pltpu.VMEM((RING - 1, BLOCKS, size, CHANNELS), jnp.bfloat16) for _, size, _ in CLASSES]
    for _ in range(2):
        scratch += [
            pltpu.VMEM((RING, RING, tables, 2, size, CHANNELS), jnp.bfloat16) for _, size, _ in CLASSES
        ]
    scratch += [pltpu.VMEM((tables, 2, 128), jnp.int32) for _ in CLASSES]
    scratch += [pltpu.VMEM((RING, tables, 2, 128), jnp.int32) for _ in CLASSES]
    scratch += [
        pltpu.VMEM((2, 128), jnp.int32),
        pltpu.SMEM((3, RING, tables, 2, 128), jnp.int32),
        dma((3,)),
        dma((3, tables)),
        dma((3, tables)),
        dma((3, RING)),
        dma((3, RING)),
        dma((3, RING)),
        dma((3,)),
        dma((3, 6)),
        dma((3, 6)),
        dma((3, RING, 2)),
        dma((3, RING, 2)),
        dma((3, RING, tables)),
        dma((3, RING, tables)),
        dma((2, 4)),
        dma((2, 4)),
        pltpu.VMEM((1, 128), jnp.int32),
        pltpu.SMEM((1, 128), jnp.int32),
        dma,
    ]
    lat, lon = mask.shape
    smem = pl.BlockSpec(memory_space=pltpu.SMEM)
    vmem = pl.BlockSpec(memory_space=pltpu.VMEM)
    free = pl.BlockSpec(memory_space=pl.ANY)
    side = jax.ShapeDtypeStruct((lat, 8, CHANNELS), jnp.bfloat16)
    row = jax.ShapeDtypeStruct((lon, CHANNELS), jnp.bfloat16)
    return pl.pallas_call(
        exchange_kernel,
        out_shape=(
            jax.ShapeDtypeStruct((RING, CORES, RING, RING, 2, ROWS, CHANNELS), jnp.bfloat16),
            side,
            side,
            row,
            row,
            jax.ShapeDtypeStruct((4, lat, lon), jnp.int32),
            jax.ShapeDtypeStruct(sources.shape, jnp.int32),
        ),
        in_specs=[smem, smem, free, vmem, vmem],
        out_specs=(free, vmem, vmem, vmem, vmem, vmem, smem),
        scratch_shapes=scratch,
        compiler_params=pltpu.CompilerParams(
            collective_id=0, has_side_effects=True, vmem_limit_bytes=EXCHANGE_VMEM
        ),
        name="exchange",
    )(positions, sources, atm, state, mask)


def lean_kernel(
    count, positions, sources, atm, state, mask,
    final, west, east, south, north, masks, slots, flag, *scratch
):
    kept, gathered, sent, out3, first = (scratch[3 * i : 3 * i + 3] for i in range(5))
    relayed = [scratch[15 + 3 * c : 18 + 3 * c] for c in range(3)]
    (ask, needs, spots, lists, heard, over1, over2, over3, over1_in, over2_in, over3_in,
     table, spot_table, list_table, ask_sem, ask_s, ask_r, list_s, list_r, smem_sem, own_sem,
     ag_s, ag_r, p2_s, p2_r, p3_s, p3_r, edge_s, edge_r, over_s, over_r, firsts, leaders, lead_sem) = scratch[24:]

    barrier = pltpu.get_barrier_semaphore()
    neighbours = [(a, o, f) for a in "xyz" for o in (1, 2, 3) for f in (0, 1)] + [("x", 0, 1)]
    for axis, offset, flip in neighbours:
        pl.semaphore_signal(barrier, 1, device_id=peer(axis, offset, flip), device_id_type=MESH)
    gx, gy = lax.axis_index("gx"), lax.axis_index("gy")
    n_gx, n_gy = lax.axis_size("gx"), lax.axis_size("gy")
    is_top = gy == n_gy - 1
    before, after = ((gx + n_gx - 1) % n_gx, gy), ((gx + 1) % n_gx, gy)
    above = (jnp.where(is_top, n_gx - 1 - gx, gx), jnp.where(is_top, gy, gy + 1))
    below = (gx, gy - 1)
    has_below = gy > 0
    for target in (before, after, above):
        pl.semaphore_signal(barrier, 1, device_id=target, device_id_type=MESH)

    @pl.when(has_below)
    def _():
        pl.semaphore_signal(barrier, 1, device_id=below, device_id_type=MESH)

    lane_of = lax.broadcasted_iota(jnp.int32, (1, 128), 1)
    zero = jnp.zeros((1, 128), jnp.int32)
    live = count[0]

    def claim(step, carry):
        taken, ask0, ask1, leader = carry
        for i in range(8):
            tile = step * 8 + i
            lane, block = where_from(positions[sources[tile]])
            mine = lane_of == jnp.where(tile < live, lane, 128)
            free = mine & (taken == 0)
            ask0 = jnp.where(free, block, ask0)
            leader = jnp.where(free, tile, leader)
            ask1 = jnp.where(mine, jnp.where(free, ask1, block), ask1)
            taken = jnp.where(mine, 1, taken)
        return taken, ask0, ask1, leader

    _, ask0, ask1, leader = lax.fori_loop(
        0, sources.shape[0] // 8, claim, (zero, zero + NOBODY, zero + NOBODY, zero)
    )
    ask[0:1] = ask0
    ask[1:2] = ask1
    firsts[...] = leader
    pl.semaphore_wait(barrier, len(neighbours) + 3 + jnp.where(has_below, 1, 0))

    def copier(src, dst, send, recv, target):
        return pltpu.make_async_remote_copy(
            src_ref=src, dst_ref=dst, send_sem=send, recv_sem=recv, device_id=target, device_id_type=MESH
        )

    def remote(*parts):
        copy = copier(*parts)
        copy.start()
        return copy

    def keep(src, dst, sem):
        copy = pltpu.make_async_copy(src, dst, sem)
        copy.start()
        return copy

    half = BLOCKS // 2
    low, high = pl.ds(0, half), pl.ds(half, half)

    def direct(c, i, offset, part):
        start, size, order = CLASSES[c]
        return remote(
            atm.at[part, pl.ds(start, size)], gathered[c].at[offset, part],
            ag_s.at[c, i], ag_r.at[c, i], peer(order[0], offset),
        )

    def forward(c, i, origin, part):
        return remote(
            gathered[c].at[origin, part], gathered[c].at[2, part],
            ag_s.at[c, i], ag_r.at[c, i], peer(CLASSES[c][2][0], origin),
        )

    rings = [[direct(c, 0, 1, low), direct(c, 1, 3, high)] for c in range(3)]
    owns = []
    for c, (start, size, _) in enumerate(CLASSES):
        owns.append(keep(atm.at[:, pl.ds(start, size)], kept[c], own_sem.at[c, 0]))
        rings[c].append(keep(atm.at[:, pl.ds(start, size)], gathered[c].at[0], own_sem.at[c, 1]))

    def edges(side, slot, target, src, dst):
        return (
            copier(src, dst, edge_s.at[0, side], edge_r.at[0, slot], target),
            copier(mask, masks.at[slot], edge_s.at[1, side], edge_r.at[1, slot], target),
        )

    last = state.shape[0] - 1
    wide = state.shape[1]
    to_before = edges(0, 1, before, state.at[:, pl.ds(0, 8)], east)
    to_after = edges(1, 0, after, state.at[:, pl.ds(wide - 8, 8)], west)
    to_below = edges(2, 3, below, state.at[0], north)
    to_fold = edges(3, 3, above, state.at[last], north)
    to_above = edges(3, 2, above, state.at[last], south)
    for copy in to_before + to_after:
        copy.start()
    for case, group in ((has_below, to_below), (is_top, to_fold), (jnp.logical_not(is_top), to_above)):

        @pl.when(case)
        def _():
            for copy in group:
                copy.start()

    asks = []
    for c, (_, _, order) in enumerate(CLASSES):
        asks.append([keep(ask, first[c].at[0], ask_sem.at[c])])
        for lane in range(1, RING * CORES):
            o3, flip = lane // CORES, lane % CORES
            asks[c].append(
                remote(ask, first[c].at[lane], ask_s.at[c, lane], ask_r.at[c, lane], peer(order[2], -o3, flip))
            )
    for c in range(3):
        rings[c] += [direct(c, 2, 1, high), direct(c, 3, 3, low)]

    def wanted(c, o1, o2, lane, rank):
        order = CLASSES[c][2]
        o3, flip = lane // CORES, lane % CORES
        return table[c, lane, rank, relative({order[0]: o1, order[1]: o2, order[2]: o3}, flip)]

    keeps = []
    for c in range(3):
        for copy in asks[c]:
            copy.wait()
        keeps.append(keep(first[c], table.at[c], smem_sem.at[0, c]))
    needs[...] = jnp.zeros_like(needs)
    for c in range(3):
        keeps[c].wait()

        def mark(lane, seen):
            seen = list(seen)
            for o2 in FAR:
                for o1 in range(RING):
                    for rank in range(2):
                        key = o1 * 32 + wanted(c, o1, o2, lane, rank)
                        seen[o2 - 1] = jnp.where(lane_of == key, 1, seen[o2 - 1])
            return tuple(seen)

        seen = lax.fori_loop(0, RING * CORES, mark, (zero, zero, zero))
        for o2 in FAR:
            row = c * 3 + o2 - 1
            needs[row : row + 1] = jnp.where((lane_of & 31) < BLOCKS, seen[o2 - 1], 0)

    need = needs[...]
    upper = lax.broadcasted_iota(jnp.int32, (128, 128), 0) < lax.broadcasted_iota(jnp.int32, (128, 128), 1)
    spot = jnp.dot(
        need.astype(jnp.float32).astype(jnp.bfloat16),
        jnp.where(upper, 1.0, 0.0).astype(jnp.bfloat16),
        preferred_element_type=jnp.float32,
    ).astype(jnp.int32)
    over1[...] = jnp.where((need > 0) & (spot >= LIST), 1, 0)
    spots[...] = jnp.clip(spot, 0, LIST - 1)
    keys = lax.broadcasted_iota(jnp.int32, (8, 128), 1).astype(jnp.float32).astype(jnp.bfloat16)
    place = lax.broadcasted_iota(jnp.int32, (128, 128), 0)
    for row in range(9):
        mine = (spot[row : row + 1] == place) & (need[row : row + 1] > 0)
        lists[row] = lax.dot_general(
            keys,
            jnp.where(mine, 1.0, 0.0).astype(jnp.bfloat16),
            (((1,), (1,)), ((), ())),
            preferred_element_type=jnp.float32,
        ).astype(jnp.int32)

    def pack3(c, o2, origins):
        def body(lane, carry):
            for o1 in origins:
                for rank in range(2):
                    which = wanted(c, o1, o2, lane, rank) & 31
                    if o2:
                        at = jnp.clip(spot_table[c * 3 + o2 - 1, o1 * 32 + which], 0, LIST - 1)
                        block = relayed[c][o2 - 1][at]
                    elif o1 == 0:
                        block = kept[c][jnp.minimum(which, BLOCKS - 1)]
                    else:
                        block = gathered[c][o1, jnp.minimum(which, BLOCKS - 1)]
                    out3[c][o2, lane, o1, rank] = block
            return carry

        lax.fori_loop(0, RING * CORES, body, 0)

    p3s = []

    def send3(c, o2, origins, part):
        start, size, order = CLASSES[c]
        span = pl.ds(origins[0], len(origins))
        for lane in range(RING * CORES):
            o3, flip = lane // CORES, lane % CORES
            at = {order[0]: span, order[1]: o2, order[2]: o3}
            dst = final.at[at["x"], flip, at["z"], at["y"], :, pl.ds(start, size)]
            src = out3[c].at[o2, lane, span]
            if lane == 0:
                p3s.append(keep(src, dst, p3_s.at[c, part, 0]))
            else:
                p3s.append(
                    remote(src, dst, p3_s.at[c, part, lane], p3_r.at[c, part, lane], peer(order[2], o3, flip))
                )

    near, rest, every = (0,), (1, 2, 3), (0, 1, 2, 3)
    spot_keep = keep(spots, spot_table, smem_sem.at[1, 0])
    for owner in owns:
        owner.wait()
    pack3(0, 0, near)
    tells = []
    for c, (_, _, order) in enumerate(CLASSES):
        for o2 in FAR:
            row = c * 3 + o2 - 1
            tells.append(
                remote(lists.at[row], heard.at[row], list_s.at[row], list_r.at[row], peer(order[1], -o2))
            )
    circle = [(o, f) for o in range(RING) for f in range(CORES) if o or f]
    votes = [
        remote(over1, over1_in.at[i], over_s.at[i], over_r.at[i], peer("x", o, f))
        for i, (o, f) in enumerate(circle)
    ]
    for c in range(3):
        for copy in rings[c][:3]:
            copy.wait()
        rings[c] = rings[c][3:] + [forward(c, 4, 1, low), forward(c, 5, 3, high)]
    pack3(1, 0, near)
    send3(0, 0, near, 4)
    pack3(2, 0, near)
    send3(1, 0, near, 4)
    for row, copy in enumerate(tells):
        copy.wait()
    list_keep = keep(heard, list_table, smem_sem.at[1, 1])
    send3(2, 0, near, 4)
    list_keep.wait()
    spot_keep.wait()
    for c in range(3):
        for copy in rings[c]:
            copy.wait()

    def pack2(c, o2):
        row = c * 3 + o2 - 1

        def body(step, carry):
            for i in range(8):
                slot = step * 8 + i
                key = list_table[row, 0, slot]
                origin = lax.shift_right_logical(key, 5)
                sent[c][o2 - 1, slot] = gathered[c][origin & 3, jnp.minimum(key & 31, BLOCKS - 1)]
            return carry

        lax.fori_loop(0, LIST // 8, body, 0)

    def send2(c, o2):
        return remote(
            sent[c].at[o2 - 1], relayed[c][o2 - 1], p2_s.at[c, o2 - 1], p2_r.at[c, o2 - 1],
            peer(CLASSES[c][2][1], o2),
        )

    steps = [(c, o2) for o2 in FAR for c in range(3)]
    pending = {}
    for i, step in enumerate(steps):
        pack2(*step)
        if i:
            pending[steps[i - 1]] = send2(*steps[i - 1])
    pack3(0, 0, rest)
    pending[steps[-1]] = send2(*steps[-1])
    for copy in votes:
        copy.wait()
    over2[...] = functools.reduce(jnp.maximum, [over1_in[i] for i in range(len(circle))], over1[...])
    pack3(1, 0, rest)
    send3(0, 0, rest, 0)
    pack3(2, 0, rest)
    send3(1, 0, rest, 0)
    votes = [
        remote(over2, over2_in.at[o - 1], over_s.at[7 + o - 1], over_r.at[7 + o - 1], peer("y", o)) for o in FAR
    ]
    send3(2, 0, rest, 0)
    keep(firsts, leaders, lead_sem).wait()
    write_slots(slots, positions, sources, leaders)
    for i, (c, o2) in enumerate(steps):
        pending[c, o2].wait()
        pack3(c, o2, every)
        send3(c, o2, every, o2)
        if i == 2:
            for copy in votes:
                copy.wait()
            over3[...] = functools.reduce(jnp.maximum, [over2_in[k] for k in range(3)], over2[...])
        if i == 3:
            votes = [
                remote(over3, over3_in.at[o - 1], over_s.at[10 + o - 1], over_r.at[10 + o - 1], peer("z", o))
                for o in FAR
            ]
    for copy in votes:
        copy.wait()
    verdict = functools.reduce(jnp.maximum, [over3_in[k] for k in range(3)], over3[...])
    flag[0] = jnp.max(verdict)
    for copy in p3s:
        copy.wait()
    for copy in edges(0, 0, before, state.at[:, pl.ds(0, 8)], west) + edges(1, 1, after, state.at[:, pl.ds(0, 8)], east):
        copy.wait()
    for copy in edges(3, 3, above, state.at[last], north):
        copy.wait()

    @pl.when(has_below)
    def _():
        for copy in edges(2, 2, below, state.at[0], south):
            copy.wait()


def lean_exchange(count, positions, sources, atm, state, mask):
    dma = pltpu.SemaphoreType.DMA
    tables = RING * CORES
    sizes = [size for _, size, _ in CLASSES]
    scratch = [pltpu.VMEM((BLOCKS, size, CHANNELS), jnp.bfloat16) for size in sizes]
    scratch += [pltpu.VMEM((RING, BLOCKS, size, CHANNELS), jnp.bfloat16) for size in sizes]
    scratch += [pltpu.VMEM((3, LIST, size, CHANNELS), jnp.bfloat16) for size in sizes]
    scratch += [pltpu.VMEM((RING, tables, RING, 2, size, CHANNELS), jnp.bfloat16) for size in sizes]
    scratch += [pltpu.VMEM((tables, 2, 128), jnp.int32) for _ in sizes]
    for size in sizes:
        scratch += [pltpu.VMEM((LIST, size, CHANNELS), jnp.bfloat16) for _ in range(3)]
    votes = pltpu.VMEM((16, 128), jnp.int32)
    scratch += [
        pltpu.VMEM((2, 128), jnp.int32),
        votes,
        votes,
        pltpu.VMEM((9, 8, 128), jnp.int32),
        pltpu.VMEM((9, 8, 128), jnp.int32),
        votes,
        votes,
        votes,
        pltpu.VMEM((7, 16, 128), jnp.int32),
        pltpu.VMEM((3, 16, 128), jnp.int32),
        pltpu.VMEM((3, 16, 128), jnp.int32),
        pltpu.SMEM((3, tables, 2, 128), jnp.int32),
        pltpu.SMEM((16, 128), jnp.int32),
        pltpu.SMEM((9, 8, 128), jnp.int32),
        dma((3,)),
        dma((3, tables)),
        dma((3, tables)),
        dma((9,)),
        dma((9,)),
        dma((2, 3)),
        dma((3, 2)),
        dma((3, 6)),
        dma((3, 6)),
        dma((3, 3)),
        dma((3, 3)),
        dma((3, RING + 1, tables)),
        dma((3, RING + 1, tables)),
        dma((2, 4)),
        dma((2, 4)),
        dma((13,)),
        dma((13,)),
        pltpu.VMEM((1, 128), jnp.int32),
        pltpu.SMEM((1, 128), jnp.int32),
        dma,
    ]
    lat, lon = mask.shape
    smem = pl.BlockSpec(memory_space=pltpu.SMEM)
    vmem = pl.BlockSpec(memory_space=pltpu.VMEM)
    free = pl.BlockSpec(memory_space=pl.ANY)
    hbm = pl.BlockSpec(memory_space=pltpu.HBM)
    side = jax.ShapeDtypeStruct((lat, 8, CHANNELS), jnp.bfloat16)
    row = jax.ShapeDtypeStruct((lon, CHANNELS), jnp.bfloat16)
    return pl.pallas_call(
        lean_kernel,
        out_shape=(
            jax.ShapeDtypeStruct((RING, CORES, RING, RING, 2, ROWS, CHANNELS), jnp.bfloat16),
            side,
            side,
            row,
            row,
            jax.ShapeDtypeStruct((4, lat, lon), jnp.int32),
            jax.ShapeDtypeStruct(sources.shape, jnp.int32),
            jax.ShapeDtypeStruct((1,), jnp.int32),
        ),
        in_specs=[smem, smem, smem, free, hbm, hbm],
        out_specs=(free, hbm, hbm, hbm, hbm, hbm, smem, smem),
        scratch_shapes=scratch,
        compiler_params=pltpu.CompilerParams(
            collective_id=1, has_side_effects=True, vmem_limit_bytes=EXCHANGE_VMEM
        ),
        name="lean_exchange",
    )(count, positions, sources, atm, state, mask)


def remap_kernel(
    count, slots, targets, weight, blocks, state, mask, mixing,
    west, east, south, north, masks, out, w_buf, x_buf, total, base, wet, w_sem, x_sem,
):
    live = count[0]
    steps = (live + GROUP - 1) // GROUP

    def copies(step, at, started=False):
        first = step * GROUP
        yield pltpu.make_async_copy(weight.at[pl.ds(first, GROUP)], w_buf.at[at], w_sem.at[at])
        for i in range(GROUP):
            slot = slots[first + i] if started else 0
            yield pltpu.make_async_copy(blocks.at[slot], x_buf.at[at, i], x_sem.at[at, i])

    def fetch(step):
        @pl.when(step < steps)
        def _():
            for copy in copies(step, lax.rem(step, DEPTH), True):
                copy.start()

    for step in range(DEPTH - 1):
        fetch(step)
    total[...] = jnp.zeros_like(total)
    stencil(state, mask, mixing, west, east, south, north, masks, base, wet)

    def body(step, carry):
        at = lax.rem(step, DEPTH)
        fetch(step + DEPTH - 1)
        for copy in copies(step, at):
            copy.wait()
        zero = jnp.zeros((ROWS, CHANNELS), jnp.bfloat16)
        right = []
        for i in range(GROUP):
            tile = step * GROUP + i
            target = jnp.where(tile < live, targets[tile], 2)
            x = x_buf[at, i]
            right.append(
                jnp.concatenate([jnp.where(target == b, x, zero) for b in range(2)], axis=1)
            )
        left = jnp.concatenate([w_buf[at, i] for i in range(GROUP)], axis=1)
        total[...] += jnp.dot(
            left, jnp.concatenate(right, axis=0), preferred_element_type=jnp.float32
        )
        return carry

    lax.fori_loop(0, steps, body, 0)
    lats, lons, _ = state.shape
    for i in range(lats):
        row = i * lons % ROWS
        b = i * lons // ROWS
        forcing = total[row : row + lons, b * CHANNELS : (b + 1) * CHANNELS]
        out[i] = (base[i] + wet[i] * forcing).astype(out.dtype)


def stencil(state, mask, mixing, west, east, south, north, masks, base, wet):
    gy, n_gy = lax.axis_index("gy"), lax.axis_size("gy")
    lats, lons, channels = state.shape
    shape = (lons, channels)

    def columns(part):
        turned = jnp.transpose(part.astype(jnp.float32))
        return [jnp.broadcast_to(turned[:, i : i + 1], shape) for i in range(part.shape[0])]

    lon = lax.broadcasted_iota(jnp.int32, shape, 0)
    reverse = jnp.where(
        lax.broadcasted_iota(jnp.int32, (lons, lons), 0) + lax.broadcasted_iota(jnp.int32, (lons, lons), 1)
        == lons - 1,
        1.0,
        0.0,
    )

    def flip(part):
        return jnp.dot(
            reverse, part, preferred_element_type=jnp.float32, precision=lax.Precision.HIGHEST
        )

    is_top = gy == n_gy - 1
    wets = columns(mask[...])
    west_wets, east_wets = columns(masks[0]), columns(masks[1])
    south_wet = jnp.where(gy == 0, 0.0, columns(masks[2])[lats - 1])
    from_north = columns(masks[3])
    north_wet = jnp.where(is_top, flip(from_north[lats - 1]), from_north[0])
    south_state = jnp.where(gy == 0, 0.0, south[...].astype(jnp.float32))
    north_plain = north[...].astype(jnp.float32)
    north_state = jnp.where(is_top, flip(north_plain), north_plain)
    states = [state[i].astype(jnp.float32) for i in range(lats)]
    scale = mixing[...]
    for i in range(lats):
        center = states[i]
        from_west = jnp.broadcast_to(west[i].astype(jnp.float32)[-1:], shape)
        from_east = jnp.broadcast_to(east[i].astype(jnp.float32)[:1], shape)
        sides = (
            (
                jnp.where(lon == 0, from_west, pltpu.roll(center, 1, 0)),
                jnp.where(lon == 0, pltpu.roll(west_wets[i], 1, 0), pltpu.roll(wets[i], 1, 0)),
            ),
            (
                jnp.where(lon == lons - 1, from_east, pltpu.roll(center, lons - 1, 0)),
                jnp.where(
                    lon == lons - 1, pltpu.roll(east_wets[i], lons - 1, 0), pltpu.roll(wets[i], lons - 1, 0)
                ),
            ),
            (south_state, south_wet) if i == 0 else (states[i - 1], wets[i - 1]),
            (north_state, north_wet) if i == lats - 1 else (states[i + 1], wets[i + 1]),
        )
        diffusion = jnp.zeros_like(center)
        for side_state, side_wet in sides:
            diffusion = diffusion + side_wet * (side_state - center)
        wet[i] = wets[i]
        base[i] = wets[i] * (center + scale * diffusion)


def remap(count, slots, targets, weight, blocks, state, mask, mixing, halo):
    smem = pl.BlockSpec(memory_space=pltpu.SMEM)
    vmem = pl.BlockSpec(memory_space=pltpu.VMEM)
    hbm = pl.BlockSpec(memory_space=pl.ANY)
    dma = pltpu.SemaphoreType.DMA
    return pl.pallas_call(
        remap_kernel,
        out_shape=jax.ShapeDtypeStruct(state.shape, state.dtype),
        in_specs=[smem, smem, smem, hbm, hbm] + [vmem] * 8,
        out_specs=vmem,
        scratch_shapes=[
            pltpu.VMEM((DEPTH, GROUP, ROWS, ROWS), jnp.bfloat16),
            pltpu.VMEM((DEPTH, GROUP, ROWS, CHANNELS), jnp.bfloat16),
            pltpu.VMEM((ROWS, 2 * CHANNELS), jnp.float32),
            pltpu.VMEM(state.shape, jnp.float32),
            pltpu.VMEM(state.shape, jnp.float32),
            dma((DEPTH,)),
            dma((DEPTH, GROUP)),
        ],
        compiler_params=pltpu.CompilerParams(vmem_limit_bytes=56 * 2**20),
        name="remap",
    )(count, slots, targets, weight, blocks, state, mask, mixing, *halo)


def local(atm_fields, atm_pos, tile_src, tile_tgt, tile_count, tile_weight, ocean_state, land_mask, mixing):
    atm = atm_fields.reshape(BLOCKS, ROWS, CHANNELS)

    def finish(blocks, west, east, south, north, masks, slots):
        return remap(
            tile_count, slots, tile_tgt, tile_weight, blocks.reshape(256, ROWS, CHANNELS),
            ocean_state, land_mask, mixing.reshape(1, CHANNELS), (west, east, south, north, masks),
        )

    *parts, over = lean_exchange(tile_count, atm_pos, tile_src, atm, ocean_state, land_mask)
    return lax.cond(
        over.reshape(()) > 0,
        lambda parts: finish(*exchange(atm_pos, tile_src, atm, ocean_state, land_mask)),
        lambda parts: finish(*parts),
        parts,
    )


def solution(mesh):
    both = ("gx", "gy")
    in_specs = (
        P(both, None),
        P(),
        P(both),
        P(both),
        P(both),
        P(both, None, None),
        P("gy", "gx", None),
        P("gy", "gx"),
        P(),
    )
    return jax.shard_map(
        local, mesh=mesh, in_specs=in_specs, out_specs=P("gy", "gx", None), check_vma=False
    )
```
